8 devices in a mesh: tp: 2 (over z, y), dp: 4 (over x, core).
Axes of the slice: x: 2, y: 2, z: 1, core: 2. Of those that a mesh axis runs over, the one named last changes fastest.
Arguments:
- x_in: bfloat16 [128, 3584], P(('dp', 'tp'))
- w_gate: bfloat16 [3584, 18944], P('dp', 'tp')
- w_up: bfloat16 [3584, 18944], P('dp', 'tp')
- w_down: bfloat16 [18944, 3584], P('tp', 'dp')
- grad_y: bfloat16 [128, 3584], P(('dp', 'tp'))
Outputs:
- output 1: bfloat16 [128, 3584], P(('dp', 'tp'))
- output 2: bfloat16 [128, 3584], P(('dp', 'tp'))
- output 3: float32 [3584, 18944], P('dp', 'tp')
- output 4: float32 [3584, 18944], P('dp', 'tp')
- output 5: float32 [18944, 3584], P('tp', 'dp')
All inputs are finite; a program needn't handle non-finite values.
Results may differ from the reference program's by a relative error of at most 0.00101.
Values are sent between devices in bfloat16 or wider.
A program may use at most 1 GiB of HBM per device.

```python
import jax
import jax.numpy as jnp

D = 3584
FF = 18944
TOKENS = 128


def setup_inputs(seed: int = 0) -> dict:
    base_key = jax.random.key(seed)
    key_list = jax.random.split(base_key, 5)
    x_in = jax.random.normal(key_list[0], (TOKENS, D), jnp.float32).astype(jnp.bfloat16)
    w_gate = (jax.random.normal(key_list[1], (D, FF), jnp.float32) * D ** -0.5).astype(jnp.bfloat16)
    w_up = (jax.random.normal(key_list[2], (D, FF), jnp.float32) * D ** -0.5).astype(jnp.bfloat16)
    w_down = (jax.random.normal(key_list[3], (FF, D), jnp.float32) * FF ** -0.5).astype(jnp.bfloat16)
    grad_y = jax.random.normal(key_list[4], (TOKENS, D), jnp.float32).astype(jnp.bfloat16)
    return {"x_in": x_in, "w_gate": w_gate, "w_up": w_up, "w_down": w_down, "grad_y": grad_y}


def reference(x_in, w_gate, w_up, w_down, grad_y):
    gate_pre = jnp.dot(x_in, w_gate, preferred_element_type=jnp.float32)
    up_pre = jnp.dot(x_in, w_up, preferred_element_type=jnp.float32)
    sig_gate = jax.nn.sigmoid(gate_pre)
    silu_gate = gate_pre * sig_gate
    hidden = (silu_gate * up_pre).astype(jnp.bfloat16)
    y_out = (x_in.astype(jnp.float32) + jnp.dot(hidden, w_down, preferred_element_type=jnp.float32)).astype(jnp.bfloat16)
    grad_h = jnp.dot(grad_y, w_down.T, preferred_element_type=jnp.float32)
    silu_deriv = sig_gate * (1.0 + gate_pre * (1.0 - sig_gate))
    grad_gate = (grad_h * up_pre * silu_deriv).astype(jnp.bfloat16)
    grad_up = (grad_h * silu_gate).astype(jnp.bfloat16)
    grad_x = (grad_y.astype(jnp.float32)
              + jnp.dot(grad_gate, w_gate.T, preferred_element_type=jnp.float32)
              + jnp.dot(grad_up, w_up.T, preferred_element_type=jnp.float32)).astype(jnp.bfloat16)
    grad_w_gate = jnp.dot(x_in.T, grad_gate, preferred_element_type=jnp.float32)
    grad_w_up = jnp.dot(x_in.T, grad_up, preferred_element_type=jnp.float32)
    grad_w_down = jnp.dot(hidden.T, grad_y, preferred_element_type=jnp.float32)
    return (y_out, grad_x, grad_w_gate, grad_w_up, grad_w_down)
```

```python
import functools

import jax
import jax.numpy as jnp
from jax import lax
from jax.experimental import pallas as pl
from jax.experimental.pallas import tpu as pltpu
from jax.sharding import PartitionSpec as P

F32 = jnp.float32
BF16 = jnp.bfloat16
CW = 256
SLOTS = 12
AHEAD = 3
KC, KD, KE = 4, 6, 8


def _dot(a, b, ca, cb):
    return lax.dot_general(a, b, (((ca,), (cb,)), ((), ())), preferred_element_type=F32)


def _exchange_kernel(nch, x_ref, gy_ref, wg_ref, wu_ref, wd_ref,
                     acc_ref, xc_out, hdd_out,
                     xc, wgb, wub, wdb, part, rdat, sx, rx, hdd,
                     wsem, tsem_s, tsem_r, ds, dr, xs, xr, gs, gr, fs, fr, osem, csem):
    dp = lax.axis_index("dp")
    tp = lax.axis_index("tp")
    xi = dp // 2
    co = dp % 2
    dd = xc.shape[2]
    mine = pl.multiple_of(co * 64, 64)
    other = pl.multiple_of((1 - co) * 64, 64)
    own = pl.multiple_of(xi * 32, 32)
    away = pl.multiple_of((1 - xi) * 32, 32)
    own_abs = pl.multiple_of(co * 64 + xi * 32, 32)
    partner = {"dp": xi * 2 + (1 - co)}
    xpeer = {"dp": (1 - xi) * 2 + co}

    def wcopies(j):
        s = j % SLOTS
        cols = pl.ds(pl.multiple_of(j * CW, CW), CW)
        return (pltpu.make_async_copy(wg_ref.at[:, cols], wgb.at[s], wsem.at[0, s]),
                pltpu.make_async_copy(wu_ref.at[:, cols], wub.at[s], wsem.at[1, s]),
                pltpu.make_async_copy(wd_ref.at[cols, :], wdb.at[s], wsem.at[2, s]))

    for j in range(AHEAD):
        for c in wcopies(j):
            c.start()

    rel = [(ax, ac, at) for ax in (0, 1) for ac in (0, 1) for at in (0, 1)][1:]

    def peer(r):
        ax, ac, at = r
        px = 1 - xi if ax else xi
        pc = 1 - co if ac else co
        pt = 1 - tp if at else tp
        return px * 2 + pc, pt

    barrier = pltpu.get_barrier_semaphore()
    for r in rel:
        q, pt = peer(r)
        pl.semaphore_signal(barrier, inc=1, device_id={"dp": q, "tp": pt},
                            device_id_type=pl.DeviceIdType.MESH)
    pl.semaphore_wait(barrier, len(rel))

    pos = pl.multiple_of(co * 64 + xi * 32 + tp * 16, 16)
    tok = []
    for n, r in enumerate(rel):
        q, pt = peer(r)
        qcols = pl.ds(pl.multiple_of(q * dd, 128), dd)
        for k, src in enumerate((x_ref, gy_ref)):
            c = pltpu.make_async_remote_copy(
                src_ref=src.at[:, qcols], dst_ref=xc.at[k, pl.ds(pos, 16), :],
                send_sem=tsem_s.at[k, n], recv_sem=tsem_r.at[k, n],
                device_id={"dp": q, "tp": pt}, device_id_type=pl.DeviceIdType.MESH)
            c.start()
            tok.append(c)
    mcols = pl.ds(pl.multiple_of(dp * dd, 128), dd)
    xc[0, pl.ds(pos, 16), :] = x_ref[:, mcols]
    xc[1, pl.ds(pos, 16), :] = gy_ref[:, mcols]
    acc_ref[...] = jnp.zeros_like(acc_ref)
    for c in tok:
        c.wait()

    def d_copy(j):
        return pltpu.make_async_remote_copy(
            src_ref=part.at[j, :, pl.ds(other, 64), :], dst_ref=rdat.at[j],
            send_sem=ds.at[j], recv_sem=dr.at[j],
            device_id=partner, device_id_type=pl.DeviceIdType.MESH)

    def x_copy(j):
        return pltpu.make_async_remote_copy(
            src_ref=sx.at[j], dst_ref=rx.at[j],
            send_sem=xs.at[j], recv_sem=xr.at[j],
            device_id=xpeer, device_id_type=pl.DeviceIdType.MESH)

    def g_copy(j):
        blk = hdd.at[j, :, pl.ds(own_abs, 32), :]
        return pltpu.make_async_remote_copy(
            src_ref=blk, dst_ref=blk, send_sem=gs.at[j], recv_sem=gr.at[j],
            device_id=xpeer, device_id_type=pl.DeviceIdType.MESH)

    def f_copy(j):
        blk = hdd.at[j, :, pl.ds(mine, 64), :]
        return pltpu.make_async_remote_copy(
            src_ref=blk, dst_ref=blk, send_sem=fs.at[j], recv_sem=fr.at[j],
            device_id=partner, device_id_type=pl.DeviceIdType.MESH)

    def o_copy(j):
        return pltpu.make_async_copy(hdd.at[j], hdd_out.at[j], osem.at[j])

    def step(i, carry):
        @pl.when(i + AHEAD < nch)
        def _():
            for c in wcopies(i + AHEAD):
                c.start()

        @pl.when(i < nch)
        def _():
            for c in wcopies(i):
                c.wait()
            s = i % SLOTS
            part[i, 0] = _dot(xc[0], wgb[s], 1, 0)
            part[i, 1] = _dot(xc[0], wub[s], 1, 0)
            part[i, 2] = _dot(xc[1], wdb[s], 1, 1)

        @pl.when((i >= KC + 1) & (i < nch + KC + 1))
        def _():
            g_copy(i - KC - 1).start()

        @pl.when((i >= 1) & (i < nch + 1))
        def _():
            j = i - 1
            d_copy(j).wait_recv()
            for k in range(3):
                sx[j, k] = (part[j, k, pl.ds(pl.multiple_of(mine + away, 32), 32), :]
                            + rdat[j, k, pl.ds(away, 32), :])

        @pl.when(i < nch)
        def _():
            d_copy(i).start()

        @pl.when((i >= KE) & (i < nch + KE))
        def _():
            j = i - KE
            s = j % SLOTS
            f_copy(j).wait_recv()
            o_copy(j).start()
            acc_ref[0] += _dot(hdd[j, 0], wdb[s], 1, 0)
            acc_ref[1] += _dot(hdd[j, 1], wgb[s], 1, 1) + _dot(hdd[j, 2], wub[s], 1, 1)

        @pl.when((i >= 1) & (i < nch + 1))
        def _():
            x_copy(i - 1).start()

        @pl.when((i >= KD) & (i < nch + KD))
        def _():
            g_copy(i - KD).wait_recv()
            f_copy(i - KD).start()

        @pl.when((i >= KC) & (i < nch + KC))
        def _():
            j = i - KC
            x_copy(j).wait_recv()
            a, b, g = (part[j, k, pl.ds(own_abs, 32), :] + rdat[j, k, pl.ds(own, 32), :] + rx[j, k]
                       for k in range(3))
            sig = jax.nn.sigmoid(a)
            silu = a * sig
            hdd[j, 0, pl.ds(own_abs, 32), :] = (silu * b).astype(BF16)
            deriv = sig * (1.0 + a * (1.0 - sig))
            hdd[j, 1, pl.ds(own_abs, 32), :] = (g * b * deriv).astype(BF16)
            hdd[j, 2, pl.ds(own_abs, 32), :] = (g * silu).astype(BF16)

        return carry

    lax.fori_loop(0, nch + KE, step, 0)

    cc = pltpu.make_async_copy(xc, xc_out, csem)
    cc.start()

    def finish(j, carry):
        d_copy(j).wait_send()
        x_copy(j).wait_send()
        g_copy(j).wait_send()
        f_copy(j).wait_send()
        o_copy(j).wait()
        return carry

    lax.fori_loop(0, nch, finish, 0)
    cc.wait()


def _exchange(x_loc, gy_loc, wg, wu, wd):
    dd, ff = wg.shape
    nch = ff // CW
    tok = 128
    vm = pl.BlockSpec(memory_space=pltpu.VMEM)
    hbm = pl.BlockSpec(memory_space=pl.ANY)
    dma = pltpu.SemaphoreType.DMA
    return pl.pallas_call(
        functools.partial(_exchange_kernel, nch),
        out_shape=(jax.ShapeDtypeStruct((2, tok, dd), F32),
                   jax.ShapeDtypeStruct((2, tok, dd), BF16),
                   jax.ShapeDtypeStruct((nch, 3, tok, CW), BF16)),
        in_specs=[vm, vm, hbm, hbm, hbm],
        out_specs=(vm, hbm, hbm),
        scratch_shapes=[
            pltpu.VMEM((2, tok, dd), BF16),
            pltpu.VMEM((SLOTS, dd, CW), BF16),
            pltpu.VMEM((SLOTS, dd, CW), BF16),
            pltpu.VMEM((SLOTS, CW, dd), BF16),
            pltpu.VMEM((nch, 3, tok, CW), F32),
            pltpu.VMEM((nch, 3, 64, CW), F32),
            pltpu.VMEM((nch, 3, 32, CW), F32),
            pltpu.VMEM((nch, 3, 32, CW), F32),
            pltpu.VMEM((nch, 3, tok, CW), BF16),
            dma((3, SLOTS)), dma((2, 7)), dma((2, 7)),
            dma((nch,)), dma((nch,)), dma((nch,)), dma((nch,)),
            dma((nch,)), dma((nch,)), dma((nch,)), dma((nch,)),
            dma((nch,)), dma(()),
        ],
        compiler_params=pltpu.CompilerParams(
            collective_id=0, has_side_effects=True, vmem_limit_bytes=66 * 1000 * 1000),
        cost_estimate=pl.CostEstimate(flops=12 * tok * dd * ff, bytes_accessed=6 * dd * ff,
                                      transcendentals=0),
        name="exchange",
    )(x_loc, gy_loc, wg, wu, wd)


def _down_kernel(gy_ref, h_ref, o_ref):
    o_ref[...] = _dot(h_ref[0, 0], gy_ref[0], 0, 0)


def _up_kernel(xt_ref, d_ref, og_ref, ou_ref):
    xt = xt_ref[...]
    og_ref[...] = _dot(xt, d_ref[0, 1], 1, 0)
    ou_ref[...] = _dot(xt, d_ref[0, 2], 1, 0)


def _grads(xc, hdd):
    nch = hdd.shape[0]
    _, tok, dd = xc.shape
    ff = nch * CW
    gwd = pl.pallas_call(
        _down_kernel,
        grid=(nch,),
        out_shape=jax.ShapeDtypeStruct((ff, dd), F32),
        in_specs=[pl.BlockSpec((1, tok, dd), lambda i: (1, 0, 0)),
                  pl.BlockSpec((1, 1, tok, CW), lambda i: (i, 0, 0, 0))],
        out_specs=pl.BlockSpec((CW, dd), lambda i: (i, 0)),
        cost_estimate=pl.CostEstimate(flops=2 * tok * dd * ff, bytes_accessed=4 * dd * ff,
                                      transcendentals=0),
        name="grad_down",
    )(xc, hdd)
    gwg, gwu = pl.pallas_call(
        _up_kernel,
        grid=(nch,),
        out_shape=(jax.ShapeDtypeStruct((dd, ff), F32), jax.ShapeDtypeStruct((dd, ff), F32)),
        in_specs=[pl.BlockSpec((dd, tok), lambda i: (0, 0)),
                  pl.BlockSpec((1, 3, tok, CW), lambda i: (i, 0, 0, 0))],
        out_specs=(pl.BlockSpec((dd, CW), lambda i: (0, i)), pl.BlockSpec((dd, CW), lambda i: (0, i))),
        cost_estimate=pl.CostEstimate(flops=4 * tok * dd * ff, bytes_accessed=8 * dd * ff,
                                      transcendentals=0),
        name="grad_up",
    )(xc[0].T, hdd)
    return gwg, gwu, gwd


def solution(mesh):
    def local_step(x_loc, wg, wu, wd, gy_loc):
        acc, xc, hdd = _exchange(x_loc, gy_loc, wg, wu, wd)
        dd = wg.shape[0]
        tp = lax.axis_index("tp")
        acc5 = acc.reshape(2, 2, 2, 2, 16, dd)
        keep = lax.dynamic_index_in_dim(acc5, tp, 3, keepdims=False)
        give = lax.dynamic_index_in_dim(acc5, 1 - tp, 3, keepdims=False)
        got = lax.ppermute(give, "tp", [(0, 1), (1, 0)])
        resid = lax.dynamic_index_in_dim(xc.reshape(2, 2, 2, 2, 16, dd), tp, 3, keepdims=False)
        rows = (keep + got + resid.astype(F32)).astype(BF16)
        rows = rows.transpose(2, 1, 0, 3, 4).reshape(4, 2, 16, dd)
        rows = lax.all_to_all(rows, "dp", 0, 0, tiled=True)
        rows = rows.transpose(1, 2, 0, 3).reshape(2, 16, 4 * dd)
        gwg, gwu, gwd = _grads(xc, hdd)
        return rows[0], rows[1], gwg, gwu, gwd

    row_spec = P(("dp", "tp"), None)
    up_spec = P("dp", "tp")
    down_spec = P("tp", "dp")
    return jax.shard_map(local_step, mesh=mesh,
                         in_specs=(row_spec, up_spec, up_spec, down_spec, row_spec),
                         out_specs=(row_spec, row_spec, up_spec, up_spec, down_spec),
                         check_vma=False)
```

```python
import functools

import jax
import jax.numpy as jnp
from jax import lax
from jax.experimental import pallas as pl
from jax.experimental.pallas import tpu as pltpu
from jax.sharding import PartitionSpec as P

F32 = jnp.float32
BF16 = jnp.bfloat16
CW = 256
SLOTS = 12
RING = 8
AHEAD = 3
KC, KD, KE = 4, 6, 7


def _dot(a, b, ca, cb):
    return lax.dot_general(a, b, (((ca,), (cb,)), ((), ())), preferred_element_type=F32)


def _exchange_kernel(nch, x_ref, gy_ref, wg_ref, wu_ref, wd_ref,
                     give, xc_out, hdd_out,
                     acc_ref, xc, wgb, wub, wdb, part, rdat, sx, rx, hdd,
                     wsem, tsem_s, tsem_r, ds, dr, xs, xr, gs, gr, fs, fr, osem, csem):
    dp = lax.axis_index("dp")
    tp = lax.axis_index("tp")
    xi = dp // 2
    co = dp % 2
    dd = xc.shape[2]
    mine = pl.multiple_of(co * 64, 64)
    other = pl.multiple_of((1 - co) * 64, 64)
    own = pl.multiple_of(xi * 32, 32)
    away = pl.multiple_of((1 - xi) * 32, 32)
    own_abs = pl.multiple_of(co * 64 + xi * 32, 32)
    partner = {"dp": xi * 2 + (1 - co)}
    xpeer = {"dp": (1 - xi) * 2 + co}

    def wcopies(j):
        s = j % SLOTS
        cols = pl.ds(pl.multiple_of(j * CW, CW), CW)
        return (pltpu.make_async_copy(wg_ref.at[:, cols], wgb.at[s], wsem.at[0, s]),
                pltpu.make_async_copy(wu_ref.at[:, cols], wub.at[s], wsem.at[1, s]),
                pltpu.make_async_copy(wd_ref.at[cols, :], wdb.at[s], wsem.at[2, s]))

    for j in range(AHEAD):
        for c in wcopies(j):
            c.start()

    rel = [(ax, ac, at) for ax in (0, 1) for ac in (0, 1) for at in (0, 1)][1:]

    def peer(r):
        ax, ac, at = r
        px = 1 - xi if ax else xi
        pc = 1 - co if ac else co
        pt = 1 - tp if at else tp
        return px * 2 + pc, pt

    barrier = pltpu.get_barrier_semaphore()
    for r in rel:
        q, pt = peer(r)
        pl.semaphore_signal(barrier, inc=1, device_id={"dp": q, "tp": pt},
                            device_id_type=pl.DeviceIdType.MESH)
    pl.semaphore_wait(barrier, len(rel))

    pos = pl.multiple_of(co * 64 + xi * 32 + tp * 16, 16)
    tok = []
    for k, src in enumerate((x_ref, gy_ref)):
        for n, r in enumerate(rel):
            q, pt = peer(r)
            qcols = pl.ds(pl.multiple_of(q * dd, 128), dd)
            c = pltpu.make_async_remote_copy(
                src_ref=src.at[:, qcols], dst_ref=xc.at[k, pl.ds(pos, 16), :],
                send_sem=tsem_s.at[k, n], recv_sem=tsem_r.at[k, n],
                device_id={"dp": q, "tp": pt}, device_id_type=pl.DeviceIdType.MESH)
            c.start()
            tok.append(c)
    mcols = pl.ds(pl.multiple_of(dp * dd, 128), dd)
    xc[0, pl.ds(pos, 16), :] = x_ref[:, mcols]
    xc[1, pl.ds(pos, 16), :] = gy_ref[:, mcols]
    acc_ref[...] = jnp.zeros_like(acc_ref)
    for c in tok[:len(rel)]:
        c.wait()

    def d_copy(j):
        return pltpu.make_async_remote_copy(
            src_ref=part.at[j, :, pl.ds(other, 64), :], dst_ref=rdat.at[j],
            send_sem=ds.at[j], recv_sem=dr.at[j],
            device_id=partner, device_id_type=pl.DeviceIdType.MESH)

    def x_copy(j):
        return pltpu.make_async_remote_copy(
            src_ref=sx.at[j], dst_ref=rx.at[j],
            send_sem=xs.at[j], recv_sem=xr.at[j],
            device_id=xpeer, device_id_type=pl.DeviceIdType.MESH)

    def g_copy(j):
        blk = hdd.at[j, :, pl.ds(own_abs, 32), :]
        return pltpu.make_async_remote_copy(
            src_ref=blk, dst_ref=blk, send_sem=gs.at[j], recv_sem=gr.at[j],
            device_id=xpeer, device_id_type=pl.DeviceIdType.MESH)

    def f_copy(j):
        blk = hdd.at[j, :, pl.ds(mine, 64), :]
        return pltpu.make_async_remote_copy(
            src_ref=blk, dst_ref=blk, send_sem=fs.at[j], recv_sem=fr.at[j],
            device_id=partner, device_id_type=pl.DeviceIdType.MESH)

    def o_copy(j):
        return pltpu.make_async_copy(hdd.at[j], hdd_out.at[j], osem.at[j])

    def step(i, carry):
        @pl.when(i + AHEAD < nch)
        def _():
            for c in wcopies(i + AHEAD):
                c.start()

        @pl.when(i < nch)
        def _():
            for c in wcopies(i):
                c.wait()
            s = i % SLOTS
            part[i, 0] = _dot(xc[0], wgb[s], 1, 0)
            part[i, 1] = _dot(xc[0], wub[s], 1, 0)

            @pl.when(i == 0)
            def _():
                for c in tok[len(rel):]:
                    c.wait()

            part[i, 2] = _dot(xc[1], wdb[s], 1, 1)

        @pl.when((i >= KC + 1) & (i < nch + KC + 1))
        def _():
            g_copy(i - KC - 1).start()

        @pl.when((i >= 1) & (i < nch + 1))
        def _():
            j = i - 1
            d_copy(j).wait_recv()
            for k in range(3):
                sx[j, k] = (part[j, k, pl.ds(pl.multiple_of(mine + away, 32), 32), :]
                            + rdat[j, k, pl.ds(away, 32), :])

        @pl.when(i < nch)
        def _():
            d_copy(i).start()

        @pl.when((i >= KE) & (i < nch + KE))
        def _():
            j = i - KE
            s = j % SLOTS
            f_copy(j).wait_recv()
            o_copy(j).start()
            acc_ref[0] += _dot(hdd[j, 0], wdb[s], 1, 0)
            acc_ref[1] += _dot(hdd[j, 1], wgb[s], 1, 1) + _dot(hdd[j, 2], wub[s], 1, 1)

        @pl.when((i >= 1) & (i < nch + 1))
        def _():
            x_copy(i - 1).start()

        @pl.when((i >= KD) & (i < nch + KD))
        def _():
            g_copy(i - KD).wait_recv()
            f_copy(i - KD).start()

        @pl.when((i >= KC) & (i < nch + KC))
        def _():
            j = i - KC
            x_copy(j).wait_recv()
            a, b, g = (part[j, k, pl.ds(own_abs, 32), :] + rdat[j, k, pl.ds(own, 32), :] + rx[j, k]
                       for k in range(3))
            sig = jax.nn.sigmoid(a)
            silu = a * sig
            hdd[j, 0, pl.ds(own_abs, 32), :] = (silu * b).astype(BF16)
            deriv = sig * (1.0 + a * (1.0 - sig))
            hdd[j, 1, pl.ds(own_abs, 32), :] = (g * b * deriv).astype(BF16)
            hdd[j, 2, pl.ds(own_abs, 32), :] = (g * silu).astype(BF16)

        return carry

    lax.fori_loop(0, nch + KE, step, 0)

    cc = pltpu.make_async_copy(xc, xc_out, csem)
    cc.start()
    for t in range(2):
        for q in range(4):
            row = (q % 2) * 64 + (q // 2) * 32 + t * 16
            give[t * 4 + q] = acc_ref[:, row:row + 16, :]

    def finish(j, carry):
        d_copy(j).wait_send()
        x_copy(j).wait_send()
        g_copy(j).wait_send()
        f_copy(j).wait_send()
        o_copy(j).wait()
        return carry

    lax.fori_loop(0, nch, finish, 0)
    cc.wait()


def _exchange(x_loc, gy_loc, wg, wu, wd):
    dd, ff = wg.shape
    nch = ff // CW
    tok = 128
    vm = pl.BlockSpec(memory_space=pltpu.VMEM)
    hbm = pl.BlockSpec(memory_space=pl.ANY)
    dma = pltpu.SemaphoreType.DMA
    return pl.pallas_call(
        functools.partial(_exchange_kernel, nch),
        out_shape=(jax.ShapeDtypeStruct((8, 2, 16, dd), F32),
                   jax.ShapeDtypeStruct((2, tok, dd), BF16),
                   jax.ShapeDtypeStruct((nch, 3, tok, CW), BF16)),
        in_specs=[vm, vm, hbm, hbm, hbm],
        out_specs=(vm, hbm, hbm),
        scratch_shapes=[
            pltpu.VMEM((2, tok, dd), F32),
            pltpu.VMEM((2, tok, dd), BF16),
            pltpu.VMEM((SLOTS, dd, CW), BF16),
            pltpu.VMEM((SLOTS, dd, CW), BF16),
            pltpu.VMEM((SLOTS, CW, dd), BF16),
            pltpu.VMEM((nch, 3, tok, CW), F32),
            pltpu.VMEM((nch, 3, 64, CW), F32),
            pltpu.VMEM((nch, 3, 32, CW), F32),
            pltpu.VMEM((nch, 3, 32, CW), F32),
            pltpu.VMEM((nch, 3, tok, CW), BF16),
            dma((3, SLOTS)), dma((2, 7)), dma((2, 7)),
            dma((nch,)), dma((nch,)), dma((nch,)), dma((nch,)),
            dma((nch,)), dma((nch,)), dma((nch,)), dma((nch,)),
            dma((nch,)), dma(()),
        ],
        compiler_params=pltpu.CompilerParams(
            collective_id=0, has_side_effects=True, vmem_limit_bytes=66 * 1000 * 1000),
        cost_estimate=pl.CostEstimate(flops=12 * tok * dd * ff, bytes_accessed=6 * dd * ff,
                                      transcendentals=0),
        name="exchange",
    )(x_loc, gy_loc, wg, wu, wd)


def _grads_kernel(nch, xc_ref, hdd_ref, gwg_ref, gwu_ref, gwd_ref,
                  hdd, xt, og, ou, od, isem, osem):
    def fetch(j):
        return pltpu.make_async_copy(hdd_ref.at[j], hdd.at[j], isem.at[j])

    def put(j):
        s = j % RING
        cols = pl.ds(pl.multiple_of(j * CW, CW), CW)
        return (pltpu.make_async_copy(og.at[s], gwg_ref.at[:, cols], osem.at[0, s]),
                pltpu.make_async_copy(ou.at[s], gwu_ref.at[:, cols], osem.at[1, s]),
                pltpu.make_async_copy(od.at[s], gwd_ref.at[cols, :], osem.at[2, s]))

    def start_fetch(j, carry):
        fetch(j).start()
        return carry

    lax.fori_loop(0, nch, start_fetch, 0)
    xt[...] = xc_ref[0].T

    def step(j, carry):
        s = j % RING

        @pl.when(j >= RING)
        def _():
            for c in put(j - RING):
                c.wait()

        fetch(j).wait()
        og[s] = _dot(xt[...], hdd[j, 1], 1, 0)
        ou[s] = _dot(xt[...], hdd[j, 2], 1, 0)
        od[s] = _dot(hdd[j, 0], xc_ref[1], 0, 0)
        for c in put(j):
            c.start()
        return carry

    lax.fori_loop(0, nch, step, 0)

    def drain(j, carry):
        for c in put(j):
            c.wait()
        return carry

    lax.fori_loop(nch - RING, nch, drain, 0)


def _grads(xc, hdd):
    nch = hdd.shape[0]
    _, tok, dd = xc.shape
    ff = nch * CW
    hbm = pl.BlockSpec(memory_space=pl.ANY)
    dma = pltpu.SemaphoreType.DMA
    return pl.pallas_call(
        functools.partial(_grads_kernel, nch),
        out_shape=(jax.ShapeDtypeStruct((dd, ff), F32), jax.ShapeDtypeStruct((dd, ff), F32),
                   jax.ShapeDtypeStruct((ff, dd), F32)),
        in_specs=[pl.BlockSpec(memory_space=pltpu.VMEM), hbm],
        out_specs=(hbm, hbm, hbm),
        scratch_shapes=[
            pltpu.VMEM(hdd.shape, BF16), pltpu.VMEM((dd, tok), BF16),
            pltpu.VMEM((RING, dd, CW), F32), pltpu.VMEM((RING, dd, CW), F32),
            pltpu.VMEM((RING, CW, dd), F32),
            dma((nch,)), dma((3, RING)),
        ],
        compiler_params=pltpu.CompilerParams(vmem_limit_bytes=66 * 1000 * 1000),
        cost_estimate=pl.CostEstimate(flops=6 * tok * dd * ff, bytes_accessed=12 * dd * ff,
                                      transcendentals=0),
        name="grads",
    )(xc, hdd)


def solution(mesh):
    def local_step(x_loc, wg, wu, wd, gy_loc):
        give, xc, hdd = _exchange(x_loc, gy_loc, wg, wu, wd)
        got = lax.all_to_all(give, ("tp", "dp"), 0, 0, tiled=True)
        gwg, gwu, gwd = _grads(xc, hdd)

        def own_rows(k, resid):
            both = [got[q, k] + got[q + 4, k] for q in range(4)]
            return (jnp.concatenate(both, axis=1) + resid.astype(F32)).astype(BF16)

        return own_rows(0, x_loc), own_rows(1, gy_loc), gwg, gwu, gwd

    row_spec = P(("dp", "tp"), None)
    up_spec = P("dp", "tp")
    down_spec = P("tp", "dp")
    return jax.shard_map(local_step, mesh=mesh,
                         in_specs=(row_spec, up_spec, up_spec, down_spec, row_spec),
                         out_specs=(row_spec, row_spec, up_spec, up_spec, down_spec),
                         check_vma=False)
```

```python
import functools

import jax
import jax.numpy as jnp
from jax import lax
from jax.experimental import pallas as pl
from jax.experimental.pallas import tpu as pltpu
from jax.sharding import PartitionSpec as P

F32 = jnp.float32
BF16 = jnp.bfloat16
CW = 256
NFULL = 26
REST_AT = 8
GRAD_VMEM = 66 * 1000 * 1000
SLOTS2 = 3
AHEAD2 = 2
SLOTS = 11
RING = 8
AHEAD = 3
KC, KD, KE = 4, 6, 7


def _dot(a, b, ca, cb):
    return lax.dot_general(a, b, (((ca,), (cb,)), ((), ())), preferred_element_type=F32)


def _sigmoid_parts(a, b, g):
    sig = jax.nn.sigmoid(a)
    silu = a * sig
    deriv = sig * (1.0 + a * (1.0 - sig))
    return (silu * b).astype(BF16), (g * b * deriv).astype(BF16), (g * silu).astype(BF16)


def _remote(src, dst, send, recv, dev):
    return pltpu.make_async_remote_copy(src_ref=src, dst_ref=dst, send_sem=send, recv_sem=recv,
                                        device_id=dev, device_id_type=pl.DeviceIdType.MESH)


def _exchange_kernel(nch, nfull, x_ref, gy_ref, wg_ref, wu_ref, wd_ref,
                     acc, xc_out, hdd_out, give_out, keep_out,
                     xc, wgb, wub, wdb, wgb2, wub2, wdb2, part, rdat, sx, rx, hdd, give, keep,
                     wsem, wsem2, tsem_s, tsem_r, ds, dr, xs, xr, gs, gr, fs, fr, osem, csem, ksem):
    nrest = nch - nfull
    dp = lax.axis_index("dp")
    tp = lax.axis_index("tp")
    xi = dp // 2
    co = dp % 2
    dd = xc.shape[2]
    mine = pl.multiple_of(co * 64, 64)
    other = pl.multiple_of((1 - co) * 64, 64)
    own = pl.multiple_of(xi * 32, 32)
    away = pl.multiple_of((1 - xi) * 32, 32)
    own_abs = pl.multiple_of(co * 64 + xi * 32, 32)
    away_abs = pl.multiple_of(co * 64 + (1 - xi) * 32, 32)
    partner = {"dp": xi * 2 + (1 - co)}
    xpeer = {"dp": (1 - xi) * 2 + co}

    def wcopies(j, s, bufs, sem):
        cols = pl.ds(pl.multiple_of(j * CW, CW), CW)
        return (pltpu.make_async_copy(wg_ref.at[:, cols], bufs[0].at[s], sem.at[0, s]),
                pltpu.make_async_copy(wu_ref.at[:, cols], bufs[1].at[s], sem.at[1, s]),
                pltpu.make_async_copy(wd_ref.at[cols, :], bufs[2].at[s], sem.at[2, s]))

    def first_w(j):
        return wcopies(j, j % SLOTS, (wgb, wub, wdb), wsem)

    def rest_w(r):
        return wcopies(nfull + r, r % SLOTS2, (wgb2, wub2, wdb2), wsem2)

    for j in range(AHEAD):
        for c in first_w(j):
            c.start()

    rel = [(ax, ac, at) for ax in (0, 1) for ac in (0, 1) for at in (0, 1)][1:]

    def peer(r):
        ax, ac, at = r
        px = 1 - xi if ax else xi
        pc = 1 - co if ac else co
        pt = 1 - tp if at else tp
        return px * 2 + pc, pt

    barrier = pltpu.get_barrier_semaphore()
    for r in rel:
        q, pt = peer(r)
        pl.semaphore_signal(barrier, inc=1, device_id={"dp": q, "tp": pt},
                            device_id_type=pl.DeviceIdType.MESH)
    pl.semaphore_wait(barrier, len(rel))

    pos = pl.multiple_of(co * 64 + xi * 32 + tp * 16, 16)
    tok = []
    for k, src in enumerate((x_ref, gy_ref)):
        for n, r in enumerate(rel):
            q, pt = peer(r)
            qcols = pl.ds(pl.multiple_of(q * dd, 128), dd)
            c = _remote(src.at[:, qcols], xc.at[k, pl.ds(pos, 16), :],
                        tsem_s.at[k, n], tsem_r.at[k, n], {"dp": q, "tp": pt})
            c.start()
            tok.append(c)
    mcols = pl.ds(pl.multiple_of(dp * dd, 128), dd)
    xc[0, pl.ds(pos, 16), :] = x_ref[:, mcols]
    xc[1, pl.ds(pos, 16), :] = gy_ref[:, mcols]
    acc[...] = jnp.zeros_like(acc)
    for c in tok[:len(rel)]:
        c.wait()

    def d_copy(j):
        return _remote(part.at[j, :, pl.ds(other, 64), :], rdat.at[j], ds.at[j], dr.at[j], partner)

    def x_copy(j):
        return _remote(sx.at[j], rx.at[j], xs.at[j], xr.at[j], xpeer)

    def g_copy(j):
        blk = hdd.at[j, :, pl.ds(own_abs, 32), :]
        return _remote(blk, blk, gs.at[j], gr.at[j], xpeer)

    def f_copy(j):
        blk = hdd.at[j, :, pl.ds(mine, 64), :]
        return _remote(blk, blk, fs.at[j], fr.at[j], partner)

    def o_copy(j):
        return pltpu.make_async_copy(hdd.at[j], hdd_out.at[j], osem.at[j])

    def k_copies(r):
        return (pltpu.make_async_copy(give.at[r], give_out.at[r], ksem.at[0, r]),
                pltpu.make_async_copy(keep.at[r], keep_out.at[r], ksem.at[1, r]))

    def step(i, carry):
        rest = i - REST_AT

        @pl.when(i + AHEAD < nfull)
        def _():
            for c in first_w(i + AHEAD):
                c.start()

        @pl.when((rest + AHEAD2 >= 0) & (rest + AHEAD2 < nrest))
        def _():
            for c in rest_w(rest + AHEAD2):
                c.start()

        @pl.when(i < nfull)
        def _():
            for c in first_w(i):
                c.wait()
            s = i % SLOTS
            part[i, 0] = _dot(xc[0], wgb[s], 1, 0)
            part[i, 1] = _dot(xc[0], wub[s], 1, 0)

            @pl.when(i == 0)
            def _():
                for c in tok[len(rel):]:
                    c.wait()

            part[i, 2] = _dot(xc[1], wdb[s], 1, 1)

        @pl.when((i >= KC + 1) & (i < nfull + KC + 1))
        def _():
            g_copy(i - KC - 1).start()

        @pl.when((i >= 1) & (i < nfull + 1))
        def _():
            j = i - 1
            d_copy(j).wait_recv()
            for k in range(3):
                sx[j, k] = part[j, k, pl.ds(away_abs, 32), :] + rdat[j, k, pl.ds(away, 32), :]

        @pl.when(i < nfull)
        def _():
            d_copy(i).start()

        @pl.when((i >= KE) & (i < nfull + KE))
        def _():
            j = i - KE
            s = j % SLOTS
            f_copy(j).wait_recv()
            o_copy(j).start()
            acc[0] += _dot(hdd[j, 0], wdb[s], 1, 0)
            acc[1] += _dot(hdd[j, 1], wgb[s], 1, 1) + _dot(hdd[j, 2], wub[s], 1, 1)

        @pl.when((i >= 1) & (i < nfull + 1))
        def _():
            x_copy(i - 1).start()

        @pl.when((rest >= 0) & (rest < nrest))
        def _():
            for c in rest_w(rest):
                c.wait()
            s = rest % SLOTS2
            j = nfull + rest
            part[j, 0] = _dot(xc[0], wgb2[s], 1, 0)
            part[j, 1] = _dot(xc[0], wub2[s], 1, 0)
            part[j, 2] = _dot(xc[1], wdb2[s], 1, 1)

        @pl.when((rest >= 2) & (rest < nrest + 2))
        def _():
            for c in k_copies(rest - 2):
                c.start()

        @pl.when((rest >= 1) & (rest < nrest + 1))
        def _():
            r = rest - 1
            j = nfull + r
            d_copy(j).wait_recv()
            for k in range(3):
                give[r, k] = part[j, k, pl.ds(away_abs, 32), :] + rdat[j, k, pl.ds(away, 32), :]
                keep[r, k] = part[j, k, pl.ds(own_abs, 32), :] + rdat[j, k, pl.ds(own, 32), :]

        @pl.when((rest >= 0) & (rest < nrest))
        def _():
            d_copy(nfull + rest).start()

        @pl.when((i >= KD) & (i < nfull + KD))
        def _():
            g_copy(i - KD).wait_recv()
            f_copy(i - KD).start()

        @pl.when((i >= KC) & (i < nfull + KC))
        def _():
            j = i - KC
            x_copy(j).wait_recv()
            vals = [part[j, k, pl.ds(own_abs, 32), :] + rdat[j, k, pl.ds(own, 32), :] + rx[j, k]
                    for k in range(3)]
            for k, v in enumerate(_sigmoid_parts(*vals)):
                hdd[j, k, pl.ds(own_abs, 32), :] = v

        return carry

    lax.fori_loop(0, nfull + KE, step, 0)

    cc = pltpu.make_async_copy(xc, xc_out, csem)
    cc.start()

    def finish_full(j, carry):
        x_copy(j).wait_send()
        g_copy(j).wait_send()
        f_copy(j).wait_send()
        o_copy(j).wait()
        return carry

    def finish_all(j, carry):
        d_copy(j).wait_send()
        return carry

    def finish_rest(r, carry):
        for c in k_copies(r):
            c.wait()
        return carry

    lax.fori_loop(0, nfull, finish_full, 0)
    lax.fori_loop(0, nch, finish_all, 0)
    lax.fori_loop(0, nrest, finish_rest, 0)
    cc.wait()


def _exchange(x_loc, gy_loc, wg, wu, wd, nfull):
    dd, ff = wg.shape
    nch = ff // CW
    nrest = nch - nfull
    tok = 128
    vm = pl.BlockSpec(memory_space=pltpu.VMEM)
    hbm = pl.BlockSpec(memory_space=pl.ANY)
    dma = pltpu.SemaphoreType.DMA
    return pl.pallas_call(
        functools.partial(_exchange_kernel, nch, nfull),
        out_shape=(jax.ShapeDtypeStruct((2, tok, dd), F32),
                   jax.ShapeDtypeStruct((2, tok, dd), BF16),
                   jax.ShapeDtypeStruct((nfull, 3, tok, CW), BF16),
                   jax.ShapeDtypeStruct((nrest, 3, 32, CW), F32),
                   jax.ShapeDtypeStruct((nrest, 3, 32, CW), F32)),
        in_specs=[vm, vm, hbm, hbm, hbm],
        out_specs=(vm, hbm, hbm, hbm, hbm),
        scratch_shapes=[
            pltpu.VMEM((2, tok, dd), BF16),
            pltpu.VMEM((SLOTS, dd, CW), BF16),
            pltpu.VMEM((SLOTS, dd, CW), BF16),
            pltpu.VMEM((SLOTS, CW, dd), BF16),
            pltpu.VMEM((SLOTS2, dd, CW), BF16),
            pltpu.VMEM((SLOTS2, dd, CW), BF16),
            pltpu.VMEM((SLOTS2, CW, dd), BF16),
            pltpu.VMEM((nch, 3, tok, CW), F32),
            pltpu.VMEM((nch, 3, 64, CW), F32),
            pltpu.VMEM((nfull, 3, 32, CW), F32),
            pltpu.VMEM((nfull, 3, 32, CW), F32),
            pltpu.VMEM((nfull, 3, tok, CW), BF16),
            pltpu.VMEM((nrest, 3, 32, CW), F32),
            pltpu.VMEM((nrest, 3, 32, CW), F32),
            dma((3, SLOTS)), dma((3, SLOTS2)), dma((2, 7)), dma((2, 7)),
            dma((nch,)), dma((nch,)), dma((nfull,)), dma((nfull,)),
            dma((nfull,)), dma((nfull,)), dma((nfull,)), dma((nfull,)),
            dma((nfull,)), dma(()), dma((2, nrest)),
        ],
        compiler_params=pltpu.CompilerParams(
            collective_id=0, has_side_effects=True, vmem_limit_bytes=66 * 1000 * 1000),
        cost_estimate=pl.CostEstimate(flops=12 * tok * dd * ff, bytes_accessed=6 * dd * ff,
                                      transcendentals=0),
        name="exchange",
    )(x_loc, gy_loc, wg, wu, wd)


def _finish_kernel(nfull, nrest, acc_in, keep, got, wg_ref, wu_ref, wd_ref,
                   give, hdd_out, acc, wgb, wub, wdb, hdd,
                   wsem, gs, gr, fs, fr, osem):
    dp = lax.axis_index("dp")
    xi = dp // 2
    co = dp % 2
    mine = pl.multiple_of(co * 64, 64)
    own_abs = pl.multiple_of(co * 64 + xi * 32, 32)
    partner = {"dp": xi * 2 + (1 - co)}
    xpeer = {"dp": (1 - xi) * 2 + co}

    def wcopies(r):
        cols = pl.ds(pl.multiple_of((nfull + r) * CW, CW), CW)
        return (pltpu.make_async_copy(wg_ref.at[:, cols], wgb.at[r], wsem.at[0, r]),
                pltpu.make_async_copy(wu_ref.at[:, cols], wub.at[r], wsem.at[1, r]),
                pltpu.make_async_copy(wd_ref.at[cols, :], wdb.at[r], wsem.at[2, r]))

    def g_copy(r):
        blk = hdd.at[r, :, pl.ds(own_abs, 32), :]
        return _remote(blk, blk, gs.at[r], gr.at[r], xpeer)

    def f_copy(r):
        blk = hdd.at[r, :, pl.ds(mine, 64), :]
        return _remote(blk, blk, fs.at[r], fr.at[r], partner)

    def o_copy(r):
        return pltpu.make_async_copy(hdd.at[r], hdd_out.at[r], osem.at[r])

    barrier = pltpu.get_barrier_semaphore()
    for dev in (partner, xpeer):
        pl.semaphore_signal(barrier, inc=1, device_id=dev, device_id_type=pl.DeviceIdType.MESH)

    def fetch(r, carry):
        for c in wcopies(r):
            c.start()
        return carry

    lax.fori_loop(0, nrest, fetch, 0)
    acc[...] = acc_in[...]
    pl.semaphore_wait(barrier, 2)

    def point(r, carry):
        @pl.when(r < nrest)
        def _():
            vals = [keep[r, k] + got[r, k] for k in range(3)]
            for k, v in enumerate(_sigmoid_parts(*vals)):
                hdd[r, k, pl.ds(own_abs, 32), :] = v

        @pl.when(r >= 1)
        def _():
            g_copy(r - 1).start()

        return carry

    lax.fori_loop(0, nrest + 1, point, 0)

    def step(i, carry):
        @pl.when(i < nrest)
        def _():
            g_copy(i).wait_recv()
            f_copy(i).start()

        @pl.when(i >= 1)
        def _():
            r = i - 1
            for c in wcopies(r):
                c.wait()
            f_copy(r).wait_recv()
            o_copy(r).start()
            acc[0] += _dot(hdd[r, 0], wdb[r], 1, 0)
            acc[1] += _dot(hdd[r, 1], wgb[r], 1, 1) + _dot(hdd[r, 2], wub[r], 1, 1)

        return carry

    lax.fori_loop(0, nrest + 1, step, 0)

    for t in range(2):
        for q in range(4):
            row = (q % 2) * 64 + (q // 2) * 32 + t * 16
            give[t * 4 + q] = acc[:, row:row + 16, :]

    def finish(r, carry):
        g_copy(r).wait_send()
        f_copy(r).wait_send()
        o_copy(r).wait()
        return carry

    lax.fori_loop(0, nrest, finish, 0)


def _finish(acc, keep, got, wg, wu, wd):
    dd, ff = wg.shape
    nrest = keep.shape[0]
    nfull = ff // CW - nrest
    tok = acc.shape[1]
    vm = pl.BlockSpec(memory_space=pltpu.VMEM)
    hbm = pl.BlockSpec(memory_space=pl.ANY)
    dma = pltpu.SemaphoreType.DMA
    return pl.pallas_call(
        functools.partial(_finish_kernel, nfull, nrest),
        out_shape=(jax.ShapeDtypeStruct((8, 2, 16, dd), F32),
                   jax.ShapeDtypeStruct((nrest, 3, tok, CW), BF16)),
        in_specs=[vm, vm, vm, hbm, hbm, hbm],
        out_specs=(vm, hbm),
        scratch_shapes=[
            pltpu.VMEM((2, tok, dd), F32),
            pltpu.VMEM((nrest, dd, CW), BF16),
            pltpu.VMEM((nrest, dd, CW), BF16),
            pltpu.VMEM((nrest, CW, dd), BF16),
            pltpu.VMEM((nrest, 3, tok, CW), BF16),
            dma((3, nrest)), dma((nrest,)), dma((nrest,)), dma((nrest,)), dma((nrest,)),
            dma((nrest,)),
        ],
        compiler_params=pltpu.CompilerParams(
            collective_id=1, has_side_effects=True, vmem_limit_bytes=60 * 1000 * 1000),
        cost_estimate=pl.CostEstimate(flops=6 * tok * dd * nrest * CW, bytes_accessed=6 * dd * nrest * CW,
                                      transcendentals=0),
        name="finish",
    )(acc, keep, got, wg, wu, wd)


def _grads_kernel(base, nch, xc_ref, hdd_ref, *refs):
    gwg_ref, gwu_ref, gwd_ref, hdd, xt, og, ou, od, isem, osem = refs[-10:]

    def fetch(j):
        return pltpu.make_async_copy(hdd_ref.at[j], hdd.at[j], isem.at[j])

    def put(j):
        s = j % RING
        cols = pl.ds(pl.multiple_of((base + j) * CW, CW), CW)
        return (pltpu.make_async_copy(og.at[s], gwg_ref.at[:, cols], osem.at[0, s]),
                pltpu.make_async_copy(ou.at[s], gwu_ref.at[:, cols], osem.at[1, s]),
                pltpu.make_async_copy(od.at[s], gwd_ref.at[cols, :], osem.at[2, s]))

    def start_fetch(j, carry):
        fetch(j).start()
        return carry

    lax.fori_loop(0, nch, start_fetch, 0)
    xt[...] = xc_ref[0].T

    def step(j, carry):
        s = j % RING

        @pl.when(j >= RING)
        def _():
            for c in put(j - RING):
                c.wait()

        fetch(j).wait()
        og[s] = _dot(xt[...], hdd[j, 1], 1, 0)
        ou[s] = _dot(xt[...], hdd[j, 2], 1, 0)
        od[s] = _dot(hdd[j, 0], xc_ref[1], 0, 0)
        for c in put(j):
            c.start()
        return carry

    lax.fori_loop(0, nch, step, 0)

    def drain(j, carry):
        for c in put(j):
            c.wait()
        return carry

    lax.fori_loop(nch - RING, nch, drain, 0)


def _grads(xc, hdd, base, ff, out=()):
    nch = hdd.shape[0]
    _, tok, dd = xc.shape
    hbm = pl.BlockSpec(memory_space=pl.ANY)
    dma = pltpu.SemaphoreType.DMA
    return pl.pallas_call(
        functools.partial(_grads_kernel, base, nch),
        out_shape=(jax.ShapeDtypeStruct((dd, ff), F32), jax.ShapeDtypeStruct((dd, ff), F32),
                   jax.ShapeDtypeStruct((ff, dd), F32)),
        in_specs=[pl.BlockSpec(memory_space=pltpu.VMEM), hbm] + [hbm] * len(out),
        out_specs=(hbm, hbm, hbm),
        input_output_aliases={2 + n: n for n in range(len(out))},
        scratch_shapes=[
            pltpu.VMEM(hdd.shape, BF16), pltpu.VMEM((dd, tok), BF16),
            pltpu.VMEM((RING, dd, CW), F32), pltpu.VMEM((RING, dd, CW), F32),
            pltpu.VMEM((RING, CW, dd), F32),
            dma((nch,)), dma((3, RING)),
        ],
        compiler_params=pltpu.CompilerParams(vmem_limit_bytes=GRAD_VMEM),
        cost_estimate=pl.CostEstimate(flops=6 * tok * dd * nch * CW, bytes_accessed=12 * dd * nch * CW,
                                      transcendentals=0),
        name="grads",
    )(xc, hdd, *out)


def solution(mesh):
    def local_step(x_loc, wg, wu, wd, gy_loc):
        ff = wg.shape[1]
        acc, xc, hdd, give, keep = _exchange(x_loc, gy_loc, wg, wu, wd, NFULL)
        got = lax.ppermute(give, "dp", [(0, 2), (1, 3), (2, 0), (3, 1)])
        grads = _grads(xc, hdd, 0, ff)
        grads, keep = lax.optimization_barrier((grads, keep))
        give, hdd = _finish(acc, keep, got, wg, wu, wd)
        got = lax.all_to_all(give, ("tp", "dp"), 0, 0, tiled=True)
        gwg, gwu, gwd = _grads(xc, hdd, NFULL, ff, grads)

        def own_rows(k, resid):
            both = [got[q, k] + got[q + 4, k] for q in range(4)]
            return (jnp.concatenate(both, axis=1) + resid.astype(F32)).astype(BF16)

        return own_rows(0, x_loc), own_rows(1, gy_loc), gwg, gwu, gwd

    row_spec = P(("dp", "tp"), None)
    up_spec = P("dp", "tp")
    down_spec = P("tp", "dp")
    return jax.shard_map(local_step, mesh=mesh,
                         in_specs=(row_spec, up_spec, up_spec, down_spec, row_spec),
                         out_specs=(row_spec, row_spec, up_spec, up_spec, down_spec),
                         check_vma=False)
```

```python
import functools

import jax
import jax.numpy as jnp
from jax import lax
from jax.experimental import pallas as pl
from jax.experimental.pallas import tpu as pltpu
from jax.sharding import PartitionSpec as P

F32 = jnp.float32
BF16 = jnp.bfloat16
CW = 256
NFULL = 26
REST_AT = 8
GRAD_VMEM = 66 * 1000 * 1000
SLOTS2 = 3
AHEAD2 = 2
SLOTS = 11
RING = 8
AHEAD = 3
KC, KD, KE = 4, 6, 7


def _dot(a, b, ca, cb):
    return lax.dot_general(a, b, (((ca,), (cb,)), ((), ())), preferred_element_type=F32)


def _sigmoid_parts(a, b, g):
    sig = jax.nn.sigmoid(a)
    silu = a * sig
    deriv = sig * (1.0 + a * (1.0 - sig))
    return (silu * b).astype(BF16), (g * b * deriv).astype(BF16), (g * silu).astype(BF16)


def _remote(src, dst, send, recv, dev):
    return pltpu.make_async_remote_copy(src_ref=src, dst_ref=dst, send_sem=send, recv_sem=recv,
                                        device_id=dev, device_id_type=pl.DeviceIdType.MESH)


def _exchange_kernel(nch, nfull, x_ref, gy_ref, wg_ref, wu_ref, wd_ref,
                     acc, xc_out, hdd_out, give_out, keep_out,
                     xc, wgb, wub, wdb, wgb2, wub2, wdb2, part, rdat, sx, rx, hdd, give, keep,
                     wsem, wsem2, tsem_s, tsem_r, ds, dr, xs, xr, gs, gr, fs, fr, osem, csem, ksem, absem):
    nrest = nch - nfull
    dp = lax.axis_index("dp")
    tp = lax.axis_index("tp")
    xi = dp // 2
    co = dp % 2
    dd = xc.shape[2]
    mine = pl.multiple_of(co * 64, 64)
    other = pl.multiple_of((1 - co) * 64, 64)
    own = pl.multiple_of(xi * 32, 32)
    away = pl.multiple_of((1 - xi) * 32, 32)
    own_abs = pl.multiple_of(co * 64 + xi * 32, 32)
    away_abs = pl.multiple_of(co * 64 + (1 - xi) * 32, 32)
    partner = {"dp": xi * 2 + (1 - co)}
    xpeer = {"dp": (1 - xi) * 2 + co}

    def wcopies(j, s, bufs, sem):
        cols = pl.ds(pl.multiple_of(j * CW, CW), CW)
        return (pltpu.make_async_copy(wg_ref.at[:, cols], bufs[0].at[s], sem.at[0, s]),
                pltpu.make_async_copy(wu_ref.at[:, cols], bufs[1].at[s], sem.at[1, s]),
                pltpu.make_async_copy(wd_ref.at[cols, :], bufs[2].at[s], sem.at[2, s]))

    def first_w(j):
        return wcopies(j, j % SLOTS, (wgb, wub, wdb), wsem)

    def rest_w(r):
        return wcopies(nfull + r, r % SLOTS2, (wgb2, wub2, wdb2), wsem2)

    for j in range(AHEAD + 1):
        for c in first_w(j):
            c.start()

    rel = [(ax, ac, at) for ax in (0, 1) for ac in (0, 1) for at in (0, 1)][1:]

    def peer(r):
        ax, ac, at = r
        px = 1 - xi if ax else xi
        pc = 1 - co if ac else co
        pt = 1 - tp if at else tp
        return px * 2 + pc, pt

    barrier = pltpu.get_barrier_semaphore()
    for r in rel:
        q, pt = peer(r)
        pl.semaphore_signal(barrier, inc=1, device_id={"dp": q, "tp": pt},
                            device_id_type=pl.DeviceIdType.MESH)
    pl.semaphore_wait(barrier, len(rel))

    pos = pl.multiple_of(co * 64 + xi * 32 + tp * 16, 16)
    tok = []
    for k, src in enumerate((x_ref, gy_ref)):
        for n, r in enumerate(rel):
            q, pt = peer(r)
            qcols = pl.ds(pl.multiple_of(q * dd, 128), dd)
            c = _remote(src.at[:, qcols], xc.at[k, pl.ds(pos, 16), :],
                        tsem_s.at[k, n], tsem_r.at[k, n], {"dp": q, "tp": pt})
            c.start()
            tok.append(c)
    mcols = pl.ds(pl.multiple_of(dp * dd, 128), dd)
    xc[0, pl.ds(pos, 16), :] = x_ref[:, mcols]
    xc[1, pl.ds(pos, 16), :] = gy_ref[:, mcols]
    acc[...] = jnp.zeros_like(acc)
    for c in tok[:len(rel)]:
        c.wait()

    def d_copy(j):
        return _remote(part.at[j, :, pl.ds(other, 64), :], rdat.at[j], ds.at[j], dr.at[j], partner)

    def x_copy(j):
        return _remote(sx.at[j], rx.at[j], xs.at[j], xr.at[j], xpeer)

    def g_copy(j):
        blk = hdd.at[j, :, pl.ds(own_abs, 32), :]
        return _remote(blk, blk, gs.at[j], gr.at[j], xpeer)

    def f_copy(j):
        blk = hdd.at[j, :, pl.ds(mine, 64), :]
        return _remote(blk, blk, fs.at[j], fr.at[j], partner)

    def o_copy(j):
        return pltpu.make_async_copy(hdd.at[j], hdd_out.at[j], osem.at[j])

    def k_copies(r):
        return (pltpu.make_async_copy(give.at[r], give_out.at[r], ksem.at[0, r]),
                pltpu.make_async_copy(keep.at[r], keep_out.at[r], ksem.at[1, r]))

    def sum_away(j, k):
        return part[j, k, pl.ds(away_abs, 32), :] + rdat[j, k, pl.ds(away, 32), :]

    for c in first_w(0):
        c.wait()
    part[0, 0] = _dot(xc[0], wgb[0], 1, 0)
    part[0, 1] = _dot(xc[0], wub[0], 1, 0)
    d_ab = _remote(part.at[0, 0:2, pl.ds(other, 64), :], rdat.at[0, 0:2], ds.at[0], absem, partner)
    d_ab.start()
    d_ab.wait_recv()
    sx[0, 0] = sum_away(0, 0)
    sx[0, 1] = sum_away(0, 1)
    _remote(sx.at[0, 0:2], rx.at[0, 0:2], xs.at[0], xr.at[0], xpeer).start()
    for c in tok[len(rel):]:
        c.wait()
    part[0, 2] = _dot(xc[1], wdb[0], 1, 1)
    d_g = _remote(part.at[0, 2:3, pl.ds(other, 64), :], rdat.at[0, 2:3], ds.at[0], dr.at[0], partner)
    d_g.start()

    def step(i, carry):
        rest = i - REST_AT

        @pl.when(i + AHEAD < nfull)
        def _():
            for c in first_w(i + AHEAD):
                c.start()

        @pl.when((rest + AHEAD2 >= 0) & (rest + AHEAD2 < nrest))
        def _():
            for c in rest_w(rest + AHEAD2):
                c.start()

        @pl.when(i < nfull)
        def _():
            for c in first_w(i):
                c.wait()
            s = i % SLOTS
            part[i, 0] = _dot(xc[0], wgb[s], 1, 0)
            part[i, 1] = _dot(xc[0], wub[s], 1, 0)

            part[i, 2] = _dot(xc[1], wdb[s], 1, 1)

        @pl.when((i >= KC + 1) & (i < nfull + KC + 1))
        def _():
            g_copy(i - KC - 1).start()

        @pl.when(i == 1)
        def _():
            d_g.wait_recv()
            sx[0, 2] = sum_away(0, 2)
            _remote(sx.at[0, 2:3], rx.at[0, 2:3], xs.at[0], xr.at[0], xpeer).start()

        @pl.when((i >= 2) & (i < nfull + 1))
        def _():
            j = i - 1
            d_copy(j).wait_recv()
            for k in range(3):
                sx[j, k] = sum_away(j, k)

        @pl.when(i < nfull)
        def _():
            d_copy(i).start()

        @pl.when((i >= KE) & (i < nfull + KE))
        def _():
            j = i - KE
            s = j % SLOTS
            f_copy(j).wait_recv()
            o_copy(j).start()
            acc[0] += _dot(hdd[j, 0], wdb[s], 1, 0)
            acc[1] += _dot(hdd[j, 1], wgb[s], 1, 1) + _dot(hdd[j, 2], wub[s], 1, 1)

        @pl.when((i >= 2) & (i < nfull + 1))
        def _():
            x_copy(i - 1).start()

        @pl.when((rest >= 0) & (rest < nrest))
        def _():
            for c in rest_w(rest):
                c.wait()
            s = rest % SLOTS2
            j = nfull + rest
            part[j, 0] = _dot(xc[0], wgb2[s], 1, 0)
            part[j, 1] = _dot(xc[0], wub2[s], 1, 0)
            part[j, 2] = _dot(xc[1], wdb2[s], 1, 1)

        @pl.when((rest >= 2) & (rest < nrest + 2))
        def _():
            for c in k_copies(rest - 2):
                c.start()

        @pl.when((rest >= 1) & (rest < nrest + 1))
        def _():
            r = rest - 1
            j = nfull + r
            d_copy(j).wait_recv()
            for k in range(3):
                give[r, k] = sum_away(j, k)
                keep[r, k] = part[j, k, pl.ds(own_abs, 32), :] + rdat[j, k, pl.ds(own, 32), :]

        @pl.when((rest >= 0) & (rest < nrest))
        def _():
            d_copy(nfull + rest).start()

        @pl.when((i >= KD) & (i < nfull + KD))
        def _():
            g_copy(i - KD).wait_recv()
            f_copy(i - KD).start()

        @pl.when((i >= KC) & (i < nfull + KC))
        def _():
            j = i - KC
            x_copy(j).wait_recv()
            vals = [part[j, k, pl.ds(own_abs, 32), :] + rdat[j, k, pl.ds(own, 32), :] + rx[j, k]
                    for k in range(3)]
            for k, v in enumerate(_sigmoid_parts(*vals)):
                hdd[j, k, pl.ds(own_abs, 32), :] = v

        return carry

    lax.fori_loop(1, nfull + KE, step, 0)

    cc = pltpu.make_async_copy(xc, xc_out, csem)
    cc.start()

    def finish_full(j, carry):
        x_copy(j).wait_send()
        g_copy(j).wait_send()
        f_copy(j).wait_send()
        o_copy(j).wait()
        return carry

    def finish_all(j, carry):
        d_copy(j).wait_send()
        return carry

    def finish_rest(r, carry):
        for c in k_copies(r):
            c.wait()
        return carry

    lax.fori_loop(0, nfull, finish_full, 0)
    lax.fori_loop(0, nch, finish_all, 0)
    lax.fori_loop(0, nrest, finish_rest, 0)
    cc.wait()


def _exchange(x_loc, gy_loc, wg, wu, wd, nfull):
    dd, ff = wg.shape
    nch = ff // CW
    nrest = nch - nfull
    tok = 128
    vm = pl.BlockSpec(memory_space=pltpu.VMEM)
    hbm = pl.BlockSpec(memory_space=pl.ANY)
    dma = pltpu.SemaphoreType.DMA
    return pl.pallas_call(
        functools.partial(_exchange_kernel, nch, nfull),
        out_shape=(jax.ShapeDtypeStruct((2, tok, dd), F32),
                   jax.ShapeDtypeStruct((2, tok, dd), BF16),
                   jax.ShapeDtypeStruct((nfull, 3, tok, CW), BF16),
                   jax.ShapeDtypeStruct((nrest, 3, 32, CW), F32),
                   jax.ShapeDtypeStruct((nrest, 3, 32, CW), F32)),
        in_specs=[vm, vm, hbm, hbm, hbm],
        out_specs=(vm, hbm, hbm, hbm, hbm),
        scratch_shapes=[
            pltpu.VMEM((2, tok, dd), BF16),
            pltpu.VMEM((SLOTS, dd, CW), BF16),
            pltpu.VMEM((SLOTS, dd, CW), BF16),
            pltpu.VMEM((SLOTS, CW, dd), BF16),
            pltpu.VMEM((SLOTS2, dd, CW), BF16),
            pltpu.VMEM((SLOTS2, dd, CW), BF16),
            pltpu.VMEM((SLOTS2, CW, dd), BF16),
            pltpu.VMEM((nch, 3, tok, CW), F32),
            pltpu.VMEM((nch, 3, 64, CW), F32),
            pltpu.VMEM((nfull, 3, 32, CW), F32),
            pltpu.VMEM((nfull, 3, 32, CW), F32),
            pltpu.VMEM((nfull, 3, tok, CW), BF16),
            pltpu.VMEM((nrest, 3, 32, CW), F32),
            pltpu.VMEM((nrest, 3, 32, CW), F32),
            dma((3, SLOTS)), dma((3, SLOTS2)), dma((2, 7)), dma((2, 7)),
            dma((nch,)), dma((nch,)), dma((nfull,)), dma((nfull,)),
            dma((nfull,)), dma((nfull,)), dma((nfull,)), dma((nfull,)),
            dma((nfull,)), dma(()), dma((2, nrest)), dma(()),
        ],
        compiler_params=pltpu.CompilerParams(
            collective_id=0, has_side_effects=True, vmem_limit_bytes=66 * 1000 * 1000),
        cost_estimate=pl.CostEstimate(flops=12 * tok * dd * ff, bytes_accessed=6 * dd * ff,
                                      transcendentals=0),
        name="exchange",
    )(x_loc, gy_loc, wg, wu, wd)


def _finish_kernel(nfull, nrest, acc_in, keep_ref, got_ref, wg_ref, wu_ref, wd_ref,
                   give, hdd_out, acc, keep, got, wgb, wub, wdb, hdd,
                   wsem, isem, asem, gs, gr, fs, fr, osem):
    dp = lax.axis_index("dp")
    xi = dp // 2
    co = dp % 2
    mine = pl.multiple_of(co * 64, 64)
    own_abs = pl.multiple_of(co * 64 + xi * 32, 32)
    partner = {"dp": xi * 2 + (1 - co)}
    xpeer = {"dp": (1 - xi) * 2 + co}

    def wcopies(r):
        cols = pl.ds(pl.multiple_of((nfull + r) * CW, CW), CW)
        return (pltpu.make_async_copy(wg_ref.at[:, cols], wgb.at[r], wsem.at[0, r]),
                pltpu.make_async_copy(wu_ref.at[:, cols], wub.at[r], wsem.at[1, r]),
                pltpu.make_async_copy(wd_ref.at[cols, :], wdb.at[r], wsem.at[2, r]))

    def g_copy(r):
        blk = hdd.at[r, :, pl.ds(own_abs, 32), :]
        return _remote(blk, blk, gs.at[r], gr.at[r], xpeer)

    def f_copy(r):
        blk = hdd.at[r, :, pl.ds(mine, 64), :]
        return _remote(blk, blk, fs.at[r], fr.at[r], partner)

    def o_copy(r):
        return pltpu.make_async_copy(hdd.at[r], hdd_out.at[r], osem.at[r])

    barrier = pltpu.get_barrier_semaphore()
    for dev in (partner, xpeer):
        pl.semaphore_signal(barrier, inc=1, device_id=dev, device_id_type=pl.DeviceIdType.MESH)

    def fetch(r, carry):
        for c in wcopies(r):
            c.start()
        return carry

    def icopies(r):
        return (pltpu.make_async_copy(keep_ref.at[r], keep.at[r], isem.at[0, r]),
                pltpu.make_async_copy(got_ref.at[r], got.at[r], isem.at[1, r]))

    def fetch_sums(r, carry):
        for c in icopies(r):
            c.start()
        return carry

    lax.fori_loop(0, nrest, fetch_sums, 0)
    acopy = pltpu.make_async_copy(acc_in, acc, asem)
    acopy.start()
    lax.fori_loop(0, nrest, fetch, 0)
    pl.semaphore_wait(barrier, 2)

    def point(r, carry):
        @pl.when(r < nrest)
        def _():
            for c in icopies(r):
                c.wait()
            vals = [keep[r, k] + got[r, k] for k in range(3)]
            for k, v in enumerate(_sigmoid_parts(*vals)):
                hdd[r, k, pl.ds(own_abs, 32), :] = v

        @pl.when(r >= 1)
        def _():
            g_copy(r - 1).start()

        return carry

    lax.fori_loop(0, nrest + 1, point, 0)
    acopy.wait()

    def step(i, carry):
        @pl.when(i < nrest)
        def _():
            g_copy(i).wait_recv()
            f_copy(i).start()

        @pl.when(i >= 1)
        def _():
            r = i - 1
            for c in wcopies(r):
                c.wait()
            f_copy(r).wait_recv()
            o_copy(r).start()
            acc[0] += _dot(hdd[r, 0], wdb[r], 1, 0)
            acc[1] += _dot(hdd[r, 1], wgb[r], 1, 1) + _dot(hdd[r, 2], wub[r], 1, 1)

        return carry

    lax.fori_loop(0, nrest + 1, step, 0)

    for t in range(2):
        for q in range(4):
            row = (q % 2) * 64 + (q // 2) * 32 + t * 16
            give[t * 4 + q] = acc[:, row:row + 16, :]

    def finish(r, carry):
        g_copy(r).wait_send()
        f_copy(r).wait_send()
        o_copy(r).wait()
        return carry

    lax.fori_loop(0, nrest, finish, 0)


def _finish(acc, keep, got, wg, wu, wd):
    dd, ff = wg.shape
    nrest = keep.shape[0]
    nfull = ff // CW - nrest
    tok = acc.shape[1]
    vm = pl.BlockSpec(memory_space=pltpu.VMEM)
    hbm = pl.BlockSpec(memory_space=pl.ANY)
    dma = pltpu.SemaphoreType.DMA
    return pl.pallas_call(
        functools.partial(_finish_kernel, nfull, nrest),
        out_shape=(jax.ShapeDtypeStruct((8, 2, 16, dd), F32),
                   jax.ShapeDtypeStruct((nrest, 3, tok, CW), BF16)),
        in_specs=[hbm] * 6,
        out_specs=(vm, hbm),
        scratch_shapes=[
            pltpu.VMEM((2, tok, dd), F32),
            pltpu.VMEM((nrest, 3, 32, CW), F32),
            pltpu.VMEM((nrest, 3, 32, CW), F32),
            pltpu.VMEM((nrest, dd, CW), BF16),
            pltpu.VMEM((nrest, dd, CW), BF16),
            pltpu.VMEM((nrest, CW, dd), BF16),
            pltpu.VMEM((nrest, 3, tok, CW), BF16),
            dma((3, nrest)), dma((2, nrest)), dma(()), dma((nrest,)), dma((nrest,)), dma((nrest,)), dma((nrest,)),
            dma((nrest,)),
        ],
        compiler_params=pltpu.CompilerParams(
            collective_id=1, has_side_effects=True, vmem_limit_bytes=66 * 1000 * 1000),
        cost_estimate=pl.CostEstimate(flops=6 * tok * dd * nrest * CW, bytes_accessed=6 * dd * nrest * CW,
                                      transcendentals=0),
        name="finish",
    )(acc, keep, got, wg, wu, wd)


def _grads_kernel(base, nch, xc_ref, hdd_ref, *refs):
    gwg_ref, gwu_ref, gwd_ref, hdd, xc, xt, og, ou, od, isem, osem, csem = refs[-12:]

    def fetch(j):
        return pltpu.make_async_copy(hdd_ref.at[j], hdd.at[j], isem.at[j])

    def put(j):
        s = j % RING
        cols = pl.ds(pl.multiple_of((base + j) * CW, CW), CW)
        return (pltpu.make_async_copy(og.at[s], gwg_ref.at[:, cols], osem.at[0, s]),
                pltpu.make_async_copy(ou.at[s], gwu_ref.at[:, cols], osem.at[1, s]),
                pltpu.make_async_copy(od.at[s], gwd_ref.at[cols, :], osem.at[2, s]))

    def start_fetch(j, carry):
        fetch(j).start()
        return carry

    ccopy = pltpu.make_async_copy(xc_ref, xc, csem)
    ccopy.start()
    lax.fori_loop(0, nch, start_fetch, 0)
    ccopy.wait()
    xt[...] = xc[0].T

    def step(j, carry):
        s = j % RING

        @pl.when(j >= RING)
        def _():
            for c in put(j - RING):
                c.wait()

        fetch(j).wait()
        og[s] = _dot(xt[...], hdd[j, 1], 1, 0)
        ou[s] = _dot(xt[...], hdd[j, 2], 1, 0)
        od[s] = _dot(hdd[j, 0], xc[1], 0, 0)
        for c in put(j):
            c.start()
        return carry

    lax.fori_loop(0, nch, step, 0)

    def drain(j, carry):
        for c in put(j):
            c.wait()
        return carry

    lax.fori_loop(nch - RING, nch, drain, 0)


def _grads(xc, hdd, base, ff, out=()):
    nch = hdd.shape[0]
    _, tok, dd = xc.shape
    hbm = pl.BlockSpec(memory_space=pl.ANY)
    dma = pltpu.SemaphoreType.DMA
    return pl.pallas_call(
        functools.partial(_grads_kernel, base, nch),
        out_shape=(jax.ShapeDtypeStruct((dd, ff), F32), jax.ShapeDtypeStruct((dd, ff), F32),
                   jax.ShapeDtypeStruct((ff, dd), F32)),
        in_specs=[hbm] * (2 + len(out)),
        out_specs=(hbm, hbm, hbm),
        input_output_aliases={2 + n: n for n in range(len(out))},
        scratch_shapes=[
            pltpu.VMEM(hdd.shape, BF16), pltpu.VMEM(xc.shape, BF16), pltpu.VMEM((dd, tok), BF16),
            pltpu.VMEM((RING, dd, CW), F32), pltpu.VMEM((RING, dd, CW), F32),
            pltpu.VMEM((RING, CW, dd), F32),
            dma((nch,)), dma((3, RING)), dma(()),
        ],
        compiler_params=pltpu.CompilerParams(vmem_limit_bytes=GRAD_VMEM),
        cost_estimate=pl.CostEstimate(flops=6 * tok * dd * nch * CW, bytes_accessed=12 * dd * nch * CW,
                                      transcendentals=0),
        name="grads",
    )(xc, hdd, *out)


def solution(mesh):
    def local_step(x_loc, wg, wu, wd, gy_loc):
        ff = wg.shape[1]
        acc, xc, hdd, give, keep = _exchange(x_loc, gy_loc, wg, wu, wd, NFULL)
        got = lax.ppermute(give, "dp", [(0, 2), (1, 3), (2, 0), (3, 1)])
        grads = _grads(xc, hdd, 0, ff)
        grads, keep = lax.optimization_barrier((grads, keep))
        give, hdd = _finish(acc, keep, got, wg, wu, wd)
        got = lax.all_to_all(give, ("tp", "dp"), 0, 0, tiled=True)
        gwg, gwu, gwd = _grads(xc, hdd, NFULL, ff, grads)

        def own_rows(k, resid):
            both = [got[q, k] + got[q + 4, k] for q in range(4)]
            return (jnp.concatenate(both, axis=1) + resid.astype(F32)).astype(BF16)

        return own_rows(0, x_loc), own_rows(1, gy_loc), gwg, gwu, gwd

    row_spec = P(("dp", "tp"), None)
    up_spec = P("dp", "tp")
    down_spec = P("tp", "dp")
    return jax.shard_map(local_step, mesh=mesh,
                         in_specs=(row_spec, up_spec, up_spec, down_spec, row_spec),
                         out_specs=(row_spec, row_spec, up_spec, up_spec, down_spec),
                         check_vma=False)
```

```python
import functools

import jax
import jax.numpy as jnp
from jax import lax
from jax.experimental import pallas as pl
from jax.experimental.pallas import tpu as pltpu
from jax.sharding import PartitionSpec as P

F32 = jnp.float32
BF16 = jnp.bfloat16
CW = 256
NFULL = 24
NTAIL = 3
REST_AT = 8
GRAD_VMEM = 67_043_328
SLOTS2 = 3
AHEAD2 = 2
SLOTS = 11
RING = 8
AHEAD = 3
KC, KD, KE = 4, 6, 7


def _dot(a, b, ca, cb):
    return lax.dot_general(a, b, (((ca,), (cb,)), ((), ())), preferred_element_type=F32)


def _sigmoid_parts(a, b, g):
    sig = jax.nn.sigmoid(a)
    silu = a * sig
    deriv = sig * (1.0 + a * (1.0 - sig))
    return (silu * b).astype(BF16), (g * b * deriv).astype(BF16), (g * silu).astype(BF16)


def _remote(src, dst, send, recv, dev):
    return pltpu.make_async_remote_copy(src_ref=src, dst_ref=dst, send_sem=send, recv_sem=recv,
                                        device_id=dev, device_id_type=pl.DeviceIdType.MESH)


def _exchange_kernel(nch, nfull, x_ref, gy_ref, wg_ref, wu_ref, wd_ref,
                     acc, xc_out, hdd_out, give_out, keep_out, got_out,
                     xc, wgb, wub, wdb, wgb2, wub2, wdb2, part, rdat, sx, rx, hdd, give, keep,
                     wsem, wsem2, tsem_s, tsem_r, ds, dr, xs, xr, gs, gr, fs, fr, osem, csem, ksem, absem,
                     ts, tr):
    nrest = nch - nfull
    dp = lax.axis_index("dp")
    tp = lax.axis_index("tp")
    xi = dp // 2
    co = dp % 2
    dd = xc.shape[2]
    mine = pl.multiple_of(co * 64, 64)
    other = pl.multiple_of((1 - co) * 64, 64)
    own = pl.multiple_of(xi * 32, 32)
    away = pl.multiple_of((1 - xi) * 32, 32)
    own_abs = pl.multiple_of(co * 64 + xi * 32, 32)
    away_abs = pl.multiple_of(co * 64 + (1 - xi) * 32, 32)
    partner = {"dp": xi * 2 + (1 - co)}
    xpeer = {"dp": (1 - xi) * 2 + co}

    def wcopies(j, s, bufs, sem):
        cols = pl.ds(pl.multiple_of(j * CW, CW), CW)
        return (pltpu.make_async_copy(wg_ref.at[:, cols], bufs[0].at[s], sem.at[0, s]),
                pltpu.make_async_copy(wu_ref.at[:, cols], bufs[1].at[s], sem.at[1, s]),
                pltpu.make_async_copy(wd_ref.at[cols, :], bufs[2].at[s], sem.at[2, s]))

    def first_w(j):
        return wcopies(j, j % SLOTS, (wgb, wub, wdb), wsem)

    def rest_w(r):
        return wcopies(nfull + r, r % SLOTS2, (wgb2, wub2, wdb2), wsem2)

    for j in range(AHEAD + 1):
        for c in first_w(j):
            c.start()

    rel = [(ax, ac, at) for ax in (0, 1) for ac in (0, 1) for at in (0, 1)][1:]

    def peer(r):
        ax, ac, at = r
        px = 1 - xi if ax else xi
        pc = 1 - co if ac else co
        pt = 1 - tp if at else tp
        return px * 2 + pc, pt

    barrier = pltpu.get_barrier_semaphore()
    for r in rel:
        q, pt = peer(r)
        pl.semaphore_signal(barrier, inc=1, device_id={"dp": q, "tp": pt},
                            device_id_type=pl.DeviceIdType.MESH)
    pl.semaphore_wait(barrier, len(rel))

    pos = pl.multiple_of(co * 64 + xi * 32 + tp * 16, 16)
    tok = []
    for k, src in enumerate((x_ref, gy_ref)):
        for n, r in enumerate(rel):
            q, pt = peer(r)
            qcols = pl.ds(pl.multiple_of(q * dd, 128), dd)
            c = _remote(src.at[:, qcols], xc.at[k, pl.ds(pos, 16), :],
                        tsem_s.at[k, n], tsem_r.at[k, n], {"dp": q, "tp": pt})
            c.start()
            tok.append(c)
    mcols = pl.ds(pl.multiple_of(dp * dd, 128), dd)
    xc[0, pl.ds(pos, 16), :] = x_ref[:, mcols]
    xc[1, pl.ds(pos, 16), :] = gy_ref[:, mcols]
    acc[...] = jnp.zeros_like(acc)
    for c in tok[:len(rel)]:
        c.wait()

    def d_copy(j):
        return _remote(part.at[j, :, pl.ds(other, 64), :], rdat.at[j], ds.at[j], dr.at[j], partner)

    def x_copy(j):
        return _remote(sx.at[j], rx.at[j], xs.at[j], xr.at[j], xpeer)

    def g_copy(j):
        blk = hdd.at[j, :, pl.ds(own_abs, 32), :]
        return _remote(blk, blk, gs.at[j], gr.at[j], xpeer)

    def f_copy(j):
        blk = hdd.at[j, :, pl.ds(mine, 64), :]
        return _remote(blk, blk, fs.at[j], fr.at[j], partner)

    def o_copy(j):
        return pltpu.make_async_copy(hdd.at[j], hdd_out.at[j], osem.at[j])

    def give_copy(r):
        return pltpu.make_async_copy(give.at[r], give_out.at[r - NTAIL], ksem.at[0, r])

    def keep_copy(r):
        return pltpu.make_async_copy(keep.at[r], keep_out.at[r], ksem.at[1, r])

    def t_copy(r):
        return _remote(give.at[r], got_out.at[r], ts.at[r], tr.at[r], xpeer)

    def sum_away(j, k):
        return part[j, k, pl.ds(away_abs, 32), :] + rdat[j, k, pl.ds(away, 32), :]

    for c in first_w(0):
        c.wait()
    part[0, 0] = _dot(xc[0], wgb[0], 1, 0)
    part[0, 1] = _dot(xc[0], wub[0], 1, 0)
    d_ab = _remote(part.at[0, 0:2, pl.ds(other, 64), :], rdat.at[0, 0:2], ds.at[0], absem, partner)
    d_ab.start()
    d_ab.wait_recv()
    sx[0, 0] = sum_away(0, 0)
    sx[0, 1] = sum_away(0, 1)
    _remote(sx.at[0, 0:2], rx.at[0, 0:2], xs.at[0], xr.at[0], xpeer).start()
    for c in tok[len(rel):]:
        c.wait()
    part[0, 2] = _dot(xc[1], wdb[0], 1, 1)
    d_g = _remote(part.at[0, 2:3, pl.ds(other, 64), :], rdat.at[0, 2:3], ds.at[0], dr.at[0], partner)
    d_g.start()

    def step(i, carry):
        rest = i - REST_AT

        @pl.when(i + AHEAD < nfull)
        def _():
            for c in first_w(i + AHEAD):
                c.start()

        @pl.when((rest + AHEAD2 >= 0) & (rest + AHEAD2 < nrest))
        def _():
            for c in rest_w(rest + AHEAD2):
                c.start()

        @pl.when(i < nfull)
        def _():
            for c in first_w(i):
                c.wait()
            s = i % SLOTS
            part[i, 0] = _dot(xc[0], wgb[s], 1, 0)
            part[i, 1] = _dot(xc[0], wub[s], 1, 0)

            part[i, 2] = _dot(xc[1], wdb[s], 1, 1)

        @pl.when((i >= KC + 1) & (i < nfull + KC + 1))
        def _():
            g_copy(i - KC - 1).start()

        @pl.when(i == nfull + KC)
        def _():
            for r in range(NTAIL):
                t_copy(r).start()

        @pl.when(i == 1)
        def _():
            d_g.wait_recv()
            sx[0, 2] = sum_away(0, 2)
            _remote(sx.at[0, 2:3], rx.at[0, 2:3], xs.at[0], xr.at[0], xpeer).start()

        @pl.when((i >= 2) & (i < nfull + 1))
        def _():
            j = i - 1
            d_copy(j).wait_recv()
            for k in range(3):
                sx[j, k] = sum_away(j, k)

        @pl.when(i < nfull)
        def _():
            d_copy(i).start()

        @pl.when((i >= KE) & (i < nfull + KE))
        def _():
            j = i - KE
            s = j % SLOTS
            f_copy(j).wait_recv()
            o_copy(j).start()
            acc[0] += _dot(hdd[j, 0], wdb[s], 1, 0)
            acc[1] += _dot(hdd[j, 1], wgb[s], 1, 1) + _dot(hdd[j, 2], wub[s], 1, 1)

        @pl.when((i >= 2) & (i < nfull + 1))
        def _():
            x_copy(i - 1).start()

        @pl.when((rest >= 0) & (rest < nrest))
        def _():
            for c in rest_w(rest):
                c.wait()
            s = rest % SLOTS2
            j = nfull + rest
            part[j, 0] = _dot(xc[0], wgb2[s], 1, 0)
            part[j, 1] = _dot(xc[0], wub2[s], 1, 0)
            part[j, 2] = _dot(xc[1], wdb2[s], 1, 1)

        @pl.when((rest >= 2) & (rest < nrest + 2))
        def _():
            keep_copy(rest - 2).start()

        @pl.when((rest >= 2 + NTAIL) & (rest < nrest + 2))
        def _():
            give_copy(rest - 2).start()

        @pl.when((rest >= 1) & (rest < nrest + 1))
        def _():
            r = rest - 1
            j = nfull + r
            d_copy(j).wait_recv()
            for k in range(3):
                give[r, k] = sum_away(j, k)
                keep[r, k] = part[j, k, pl.ds(own_abs, 32), :] + rdat[j, k, pl.ds(own, 32), :]

        @pl.when((rest >= 0) & (rest < nrest))
        def _():
            d_copy(nfull + rest).start()

        @pl.when((i >= KD) & (i < nfull + KD))
        def _():
            g_copy(i - KD).wait_recv()
            f_copy(i - KD).start()

        @pl.when((i >= KC) & (i < nfull + KC))
        def _():
            j = i - KC
            x_copy(j).wait_recv()
            vals = [part[j, k, pl.ds(own_abs, 32), :] + rdat[j, k, pl.ds(own, 32), :] + rx[j, k]
                    for k in range(3)]
            for k, v in enumerate(_sigmoid_parts(*vals)):
                hdd[j, k, pl.ds(own_abs, 32), :] = v

        return carry

    lax.fori_loop(1, nfull + KE, step, 0)

    cc = pltpu.make_async_copy(xc, xc_out, csem)
    cc.start()

    def finish_full(j, carry):
        x_copy(j).wait_send()
        g_copy(j).wait_send()
        f_copy(j).wait_send()
        o_copy(j).wait()
        return carry

    def finish_all(j, carry):
        d_copy(j).wait_send()
        return carry

    def finish_keep(r, carry):
        keep_copy(r).wait()
        return carry

    def finish_give(r, carry):
        give_copy(r).wait()
        return carry

    lax.fori_loop(0, nfull, finish_full, 0)
    lax.fori_loop(0, nch, finish_all, 0)
    lax.fori_loop(0, nrest, finish_keep, 0)
    lax.fori_loop(NTAIL, nrest, finish_give, 0)
    for r in range(NTAIL):
        t_copy(r).wait()
    cc.wait()


def _exchange(x_loc, gy_loc, wg, wu, wd, nfull):
    dd, ff = wg.shape
    nch = ff // CW
    nrest = nch - nfull
    tok = 128
    vm = pl.BlockSpec(memory_space=pltpu.VMEM)
    hbm = pl.BlockSpec(memory_space=pl.ANY)
    dma = pltpu.SemaphoreType.DMA
    return pl.pallas_call(
        functools.partial(_exchange_kernel, nch, nfull),
        out_shape=(jax.ShapeDtypeStruct((2, tok, dd), F32),
                   jax.ShapeDtypeStruct((2, tok, dd), BF16),
                   jax.ShapeDtypeStruct((nfull, 3, tok, CW), BF16),
                   jax.ShapeDtypeStruct((nrest - NTAIL, 3, 32, CW), F32),
                   jax.ShapeDtypeStruct((nrest, 3, 32, CW), F32),
                   jax.ShapeDtypeStruct((NTAIL, 3, 32, CW), F32)),
        in_specs=[vm, vm, hbm, hbm, hbm],
        out_specs=(vm, hbm, hbm, hbm, hbm, hbm),
        scratch_shapes=[
            pltpu.VMEM((2, tok, dd), BF16),
            pltpu.VMEM((SLOTS, dd, CW), BF16),
            pltpu.VMEM((SLOTS, dd, CW), BF16),
            pltpu.VMEM((SLOTS, CW, dd), BF16),
            pltpu.VMEM((SLOTS2, dd, CW), BF16),
            pltpu.VMEM((SLOTS2, dd, CW), BF16),
            pltpu.VMEM((SLOTS2, CW, dd), BF16),
            pltpu.VMEM((nch, 3, tok, CW), F32),
            pltpu.VMEM((nch, 3, 64, CW), F32),
            pltpu.VMEM((nfull, 3, 32, CW), F32),
            pltpu.VMEM((nfull, 3, 32, CW), F32),
            pltpu.VMEM((nfull, 3, tok, CW), BF16),
            pltpu.VMEM((nrest, 3, 32, CW), F32),
            pltpu.VMEM((nrest, 3, 32, CW), F32),
            dma((3, SLOTS)), dma((3, SLOTS2)), dma((2, 7)), dma((2, 7)),
            dma((nch,)), dma((nch,)), dma((nfull,)), dma((nfull,)),
            dma((nfull,)), dma((nfull,)), dma((nfull,)), dma((nfull,)),
            dma((nfull,)), dma(()), dma((2, nrest)), dma(()), dma((NTAIL,)), dma((NTAIL,)),
        ],
        compiler_params=pltpu.CompilerParams(
            collective_id=0, has_side_effects=True, vmem_limit_bytes=66 * 1000 * 1000),
        cost_estimate=pl.CostEstimate(flops=12 * tok * dd * ff, bytes_accessed=6 * dd * ff,
                                      transcendentals=0),
        name="exchange",
    )(x_loc, gy_loc, wg, wu, wd)


def _finish_kernel(nfull, nrest, acc_in, keep_ref, tail_ref, got_ref, wg_ref, wu_ref, wd_ref,
                   give, hdd_out, acc, keep, got, wgb, wub, wdb, hdd,
                   wsem, isem, asem, gs, gr, fs, fr, osem):
    dp = lax.axis_index("dp")
    xi = dp // 2
    co = dp % 2
    mine = pl.multiple_of(co * 64, 64)
    own_abs = pl.multiple_of(co * 64 + xi * 32, 32)
    partner = {"dp": xi * 2 + (1 - co)}
    xpeer = {"dp": (1 - xi) * 2 + co}

    def wcopies(r):
        cols = pl.ds(pl.multiple_of((nfull + r) * CW, CW), CW)
        return (pltpu.make_async_copy(wg_ref.at[:, cols], wgb.at[r], wsem.at[0, r]),
                pltpu.make_async_copy(wu_ref.at[:, cols], wub.at[r], wsem.at[1, r]),
                pltpu.make_async_copy(wd_ref.at[cols, :], wdb.at[r], wsem.at[2, r]))

    def g_copy(r):
        blk = hdd.at[r, :, pl.ds(own_abs, 32), :]
        return _remote(blk, blk, gs.at[r], gr.at[r], xpeer)

    def f_copy(r):
        blk = hdd.at[r, :, pl.ds(mine, 64), :]
        return _remote(blk, blk, fs.at[r], fr.at[r], partner)

    def o_copy(r):
        return pltpu.make_async_copy(hdd.at[r], hdd_out.at[r], osem.at[r])

    barrier = pltpu.get_barrier_semaphore()
    for dev in (partner, xpeer):
        pl.semaphore_signal(barrier, inc=1, device_id=dev, device_id_type=pl.DeviceIdType.MESH)

    def fetch(r, carry):
        for c in wcopies(r):
            c.start()
        return carry

    def keep_in(r):
        return pltpu.make_async_copy(keep_ref.at[r], keep.at[r], isem.at[0, r])

    def got_in(r, src, at):
        return pltpu.make_async_copy(src.at[at], got.at[r], isem.at[1, r])

    for r in range(NTAIL):
        keep_in(r).start()
        got_in(r, tail_ref, r).start()

    def fetch_sums(r, carry):
        keep_in(r).start()
        got_in(r, got_ref, r - NTAIL).start()
        return carry

    lax.fori_loop(NTAIL, nrest, fetch_sums, 0)
    acopy = pltpu.make_async_copy(acc_in, acc, asem)
    acopy.start()
    lax.fori_loop(0, nrest, fetch, 0)
    pl.semaphore_wait(barrier, 2)

    def point(r, carry):
        @pl.when(r < nrest)
        def _():
            keep_in(r).wait()
            got_in(r, got_ref, 0).wait()
            vals = [keep[r, k] + got[r, k] for k in range(3)]
            for k, v in enumerate(_sigmoid_parts(*vals)):
                hdd[r, k, pl.ds(own_abs, 32), :] = v

        @pl.when(r >= 1)
        def _():
            g_copy(r - 1).start()

        return carry

    lax.fori_loop(0, nrest + 1, point, 0)
    acopy.wait()

    def step(i, carry):
        @pl.when(i < nrest)
        def _():
            g_copy(i).wait_recv()
            f_copy(i).start()

        @pl.when(i >= 1)
        def _():
            r = i - 1
            for c in wcopies(r):
                c.wait()
            f_copy(r).wait_recv()
            o_copy(r).start()
            acc[0] += _dot(hdd[r, 0], wdb[r], 1, 0)
            acc[1] += _dot(hdd[r, 1], wgb[r], 1, 1) + _dot(hdd[r, 2], wub[r], 1, 1)

        return carry

    lax.fori_loop(0, nrest + 1, step, 0)

    for t in range(2):
        for q in range(4):
            row = (q % 2) * 64 + (q // 2) * 32 + t * 16
            give[t * 4 + q] = acc[:, row:row + 16, :]

    def finish(r, carry):
        g_copy(r).wait_send()
        f_copy(r).wait_send()
        o_copy(r).wait()
        return carry

    lax.fori_loop(0, nrest, finish, 0)


def _finish(acc, keep, tail, got, wg, wu, wd):
    dd, ff = wg.shape
    nrest = keep.shape[0]
    nfull = ff // CW - nrest
    tok = acc.shape[1]
    vm = pl.BlockSpec(memory_space=pltpu.VMEM)
    hbm = pl.BlockSpec(memory_space=pl.ANY)
    dma = pltpu.SemaphoreType.DMA
    return pl.pallas_call(
        functools.partial(_finish_kernel, nfull, nrest),
        out_shape=(jax.ShapeDtypeStruct((8, 2, 16, dd), F32),
                   jax.ShapeDtypeStruct((nrest, 3, tok, CW), BF16)),
        in_specs=[hbm] * 7,
        out_specs=(vm, hbm),
        scratch_shapes=[
            pltpu.VMEM((2, tok, dd), F32),
            pltpu.VMEM((nrest, 3, 32, CW), F32),
            pltpu.VMEM((nrest, 3, 32, CW), F32),
            pltpu.VMEM((nrest, dd, CW), BF16),
            pltpu.VMEM((nrest, dd, CW), BF16),
            pltpu.VMEM((nrest, CW, dd), BF16),
            pltpu.VMEM((nrest, 3, tok, CW), BF16),
            dma((3, nrest)), dma((2, nrest)), dma(()), dma((nrest,)), dma((nrest,)), dma((nrest,)), dma((nrest,)),
            dma((nrest,)),
        ],
        compiler_params=pltpu.CompilerParams(
            collective_id=1, has_side_effects=True, vmem_limit_bytes=66 * 1000 * 1000),
        cost_estimate=pl.CostEstimate(flops=6 * tok * dd * nrest * CW, bytes_accessed=6 * dd * nrest * CW,
                                      transcendentals=0),
        name="finish",
    )(acc, keep, tail, got, wg, wu, wd)


def _grads_kernel(base, nch, xc_ref, hdd_ref, *refs):
    gwg_ref, gwu_ref, gwd_ref, hdd, xc, xt, og, ou, od, isem, osem, csem = refs[-12:]

    def fetch(j):
        return pltpu.make_async_copy(hdd_ref.at[j], hdd.at[j], isem.at[j])

    def put(j):
        s = j % RING
        cols = pl.ds(pl.multiple_of((base + j) * CW, CW), CW)
        return (pltpu.make_async_copy(og.at[s], gwg_ref.at[:, cols], osem.at[0, s]),
                pltpu.make_async_copy(ou.at[s], gwu_ref.at[:, cols], osem.at[1, s]),
                pltpu.make_async_copy(od.at[s], gwd_ref.at[cols, :], osem.at[2, s]))

    def start_fetch(j, carry):
        fetch(j).start()
        return carry

    ccopy = pltpu.make_async_copy(xc_ref, xc, csem)
    ccopy.start()
    lax.fori_loop(0, nch, start_fetch, 0)
    ccopy.wait()
    xt[...] = xc[0].T

    def step(j, carry):
        s = j % RING

        @pl.when(j >= RING)
        def _():
            for c in put(j - RING):
                c.wait()

        fetch(j).wait()
        og[s] = _dot(xt[...], hdd[j, 1], 1, 0)
        ou[s] = _dot(xt[...], hdd[j, 2], 1, 0)
        od[s] = _dot(hdd[j, 0], xc[1], 0, 0)
        for c in put(j):
            c.start()
        return carry

    lax.fori_loop(0, nch, step, 0)

    def drain(j, carry):
        for c in put(j):
            c.wait()
        return carry

    lax.fori_loop(nch - RING, nch, drain, 0)


def _grads(xc, hdd, base, ff, out=()):
    nch = hdd.shape[0]
    _, tok, dd = xc.shape
    hbm = pl.BlockSpec(memory_space=pl.ANY)
    dma = pltpu.SemaphoreType.DMA
    return pl.pallas_call(
        functools.partial(_grads_kernel, base, nch),
        out_shape=(jax.ShapeDtypeStruct((dd, ff), F32), jax.ShapeDtypeStruct((dd, ff), F32),
                   jax.ShapeDtypeStruct((ff, dd), F32)),
        in_specs=[hbm] * (2 + len(out)),
        out_specs=(hbm, hbm, hbm),
        input_output_aliases={2 + n: n for n in range(len(out))},
        scratch_shapes=[
            pltpu.VMEM(hdd.shape, BF16), pltpu.VMEM(xc.shape, BF16), pltpu.VMEM((dd, tok), BF16),
            pltpu.VMEM((RING, dd, CW), F32), pltpu.VMEM((RING, dd, CW), F32),
            pltpu.VMEM((RING, CW, dd), F32),
            dma((nch,)), dma((3, RING)), dma(()),
        ],
        compiler_params=pltpu.CompilerParams(vmem_limit_bytes=66_000_000 if out else GRAD_VMEM),
        cost_estimate=pl.CostEstimate(flops=6 * tok * dd * nch * CW, bytes_accessed=12 * dd * nch * CW,
                                      transcendentals=0),
        name="grads",
    )(xc, hdd, *out)


def solution(mesh):
    def local_step(x_loc, wg, wu, wd, gy_loc):
        ff = wg.shape[1]
        acc, xc, hdd, give, keep, tail = _exchange(x_loc, gy_loc, wg, wu, wd, NFULL)
        got = lax.ppermute(give, "dp", [(0, 2), (1, 3), (2, 0), (3, 1)])
        grads = _grads(xc, hdd, 0, ff)
        grads, keep = lax.optimization_barrier((grads, keep))
        give, hdd = _finish(acc, keep, tail, got, wg, wu, wd)
        got = lax.all_to_all(give, ("tp", "dp"), 0, 0, tiled=True)
        gwg, gwu, gwd = _grads(xc, hdd, NFULL, ff, grads)

        def own_rows(k, resid):
            both = [got[q, k] + got[q + 4, k] for q in range(4)]
            return (jnp.concatenate(both, axis=1) + resid.astype(F32)).astype(BF16)

        return own_rows(0, x_loc), own_rows(1, gy_loc), gwg, gwu, gwd

    row_spec = P(("dp", "tp"), None)
    up_spec = P("dp", "tp")
    down_spec = P("tp", "dp")
    return jax.shard_map(local_step, mesh=mesh,
                         in_specs=(row_spec, up_spec, up_spec, down_spec, row_spec),
                         out_specs=(row_spec, row_spec, up_spec, up_spec, down_spec),
                         check_vma=False)
```

```python
import functools

import jax
import jax.numpy as jnp
from jax import lax
from jax.experimental import pallas as pl
from jax.experimental.pallas import tpu as pltpu
from jax.sharding import PartitionSpec as P

F32 = jnp.float32
BF16 = jnp.bfloat16
CW = 256
NFULL = 24
NTAIL = 3
REST_AT = 8
GRAD_VMEM = 67_043_328
SLOTS2 = 3
AHEAD2 = 2
SLOTS = 11
RING = 8
AHEAD = 3
KC, KD, KE = 4, 6, 7


def _dot(a, b, ca, cb):
    return lax.dot_general(a, b, (((ca,), (cb,)), ((), ())), preferred_element_type=F32)


def _sigmoid_parts(a, b, g):
    sig = jax.nn.sigmoid(a)
    silu = a * sig
    deriv = sig * (1.0 + a * (1.0 - sig))
    return (silu * b).astype(BF16), (g * b * deriv).astype(BF16), (g * silu).astype(BF16)


def _remote(src, dst, send, recv, dev):
    return pltpu.make_async_remote_copy(src_ref=src, dst_ref=dst, send_sem=send, recv_sem=recv,
                                        device_id=dev, device_id_type=pl.DeviceIdType.MESH)


def _exchange_kernel(nch, nfull, x_in, gy_in, wg_ref, wu_ref, wd_ref,
                     acc_out, xc_out, hdd_out, give_out, keep_out, got_out,
                     acc, x_ref, gy_ref, xc, wgb, wub, wdb, wgb2, wub2, wdb2, part, rdat, sx, rx, hdd, give, keep,
                     wsem, wsem2, tsem_s, tsem_r, ds, dr, xs, xr, gs, gr, fs, fr, osem, csem, ksem, absem,
                     ts, tr, rsem, asem):
    nrest = nch - nfull
    dp = lax.axis_index("dp")
    tp = lax.axis_index("tp")
    xi = dp // 2
    co = dp % 2
    dd = xc.shape[2]
    mine = pl.multiple_of(co * 64, 64)
    other = pl.multiple_of((1 - co) * 64, 64)
    own = pl.multiple_of(xi * 32, 32)
    away = pl.multiple_of((1 - xi) * 32, 32)
    own_abs = pl.multiple_of(co * 64 + xi * 32, 32)
    away_abs = pl.multiple_of(co * 64 + (1 - xi) * 32, 32)
    partner = {"dp": xi * 2 + (1 - co)}
    xpeer = {"dp": (1 - xi) * 2 + co}

    def wcopies(j, s, bufs, sem):
        cols = pl.ds(pl.multiple_of(j * CW, CW), CW)
        return (pltpu.make_async_copy(wg_ref.at[:, cols], bufs[0].at[s], sem.at[0, s]),
                pltpu.make_async_copy(wu_ref.at[:, cols], bufs[1].at[s], sem.at[1, s]),
                pltpu.make_async_copy(wd_ref.at[cols, :], bufs[2].at[s], sem.at[2, s]))

    def first_w(j):
        return wcopies(j, j % SLOTS, (wgb, wub, wdb), wsem)

    def rest_w(r):
        return wcopies(nfull + r, r % SLOTS2, (wgb2, wub2, wdb2), wsem2)

    rows = [pltpu.make_async_copy(x_in, x_ref, rsem.at[0]),
            pltpu.make_async_copy(gy_in, gy_ref, rsem.at[1])]
    for c in rows:
        c.start()
    for j in range(AHEAD + 1):
        for c in first_w(j):
            c.start()

    rel = [(ax, ac, at) for ax in (0, 1) for ac in (0, 1) for at in (0, 1)][1:]

    def peer(r):
        ax, ac, at = r
        px = 1 - xi if ax else xi
        pc = 1 - co if ac else co
        pt = 1 - tp if at else tp
        return px * 2 + pc, pt

    barrier = pltpu.get_barrier_semaphore()
    for r in rel:
        q, pt = peer(r)
        pl.semaphore_signal(barrier, inc=1, device_id={"dp": q, "tp": pt},
                            device_id_type=pl.DeviceIdType.MESH)
    pl.semaphore_wait(barrier, len(rel))

    pos = pl.multiple_of(co * 64 + xi * 32 + tp * 16, 16)
    tok = []
    for k, src in enumerate((x_ref, gy_ref)):
        rows[k].wait()
        for n, r in enumerate(rel):
            q, pt = peer(r)
            qcols = pl.ds(pl.multiple_of(q * dd, 128), dd)
            c = _remote(src.at[:, qcols], xc.at[k, pl.ds(pos, 16), :],
                        tsem_s.at[k, n], tsem_r.at[k, n], {"dp": q, "tp": pt})
            c.start()
            tok.append(c)
    mcols = pl.ds(pl.multiple_of(dp * dd, 128), dd)
    xc[0, pl.ds(pos, 16), :] = x_ref[:, mcols]
    xc[1, pl.ds(pos, 16), :] = gy_ref[:, mcols]
    acc[...] = jnp.zeros_like(acc)
    for c in tok[:len(rel)]:
        c.wait()

    def d_copy(j):
        return _remote(part.at[j, :, pl.ds(other, 64), :], rdat.at[j], ds.at[j], dr.at[j], partner)

    def x_copy(j):
        return _remote(sx.at[j], rx.at[j], xs.at[j], xr.at[j], xpeer)

    def g_copy(j):
        blk = hdd.at[j, :, pl.ds(own_abs, 32), :]
        return _remote(blk, blk, gs.at[j], gr.at[j], xpeer)

    def f_copy(j):
        blk = hdd.at[j, :, pl.ds(mine, 64), :]
        return _remote(blk, blk, fs.at[j], fr.at[j], partner)

    def o_copy(j):
        return pltpu.make_async_copy(hdd.at[j], hdd_out.at[j], osem.at[j])

    def give_copy(r):
        return pltpu.make_async_copy(give.at[r], give_out.at[r - NTAIL], ksem.at[0, r])

    def keep_copy(r):
        return pltpu.make_async_copy(keep.at[r], keep_out.at[r], ksem.at[1, r])

    def t_copy(r):
        return _remote(give.at[r], got_out.at[r], ts.at[r], tr.at[r], xpeer)

    def sum_away(j, k):
        return part[j, k, pl.ds(away_abs, 32), :] + rdat[j, k, pl.ds(away, 32), :]

    for c in first_w(0):
        c.wait()
    part[0, 0] = _dot(xc[0], wgb[0], 1, 0)
    part[0, 1] = _dot(xc[0], wub[0], 1, 0)
    d_ab = _remote(part.at[0, 0:2, pl.ds(other, 64), :], rdat.at[0, 0:2], ds.at[0], absem, partner)
    d_ab.start()
    d_ab.wait_recv()
    sx[0, 0] = sum_away(0, 0)
    sx[0, 1] = sum_away(0, 1)
    _remote(sx.at[0, 0:2], rx.at[0, 0:2], xs.at[0], xr.at[0], xpeer).start()
    for c in tok[len(rel):]:
        c.wait()
    part[0, 2] = _dot(xc[1], wdb[0], 1, 1)
    d_g = _remote(part.at[0, 2:3, pl.ds(other, 64), :], rdat.at[0, 2:3], ds.at[0], dr.at[0], partner)
    d_g.start()

    def step(i, carry):
        rest = i - REST_AT

        @pl.when(i + AHEAD < nfull)
        def _():
            for c in first_w(i + AHEAD):
                c.start()

        @pl.when((rest + AHEAD2 >= 0) & (rest + AHEAD2 < nrest))
        def _():
            for c in rest_w(rest + AHEAD2):
                c.start()

        @pl.when(i < nfull)
        def _():
            for c in first_w(i):
                c.wait()
            s = i % SLOTS
            part[i, 0] = _dot(xc[0], wgb[s], 1, 0)
            part[i, 1] = _dot(xc[0], wub[s], 1, 0)

            part[i, 2] = _dot(xc[1], wdb[s], 1, 1)

        @pl.when((i >= KC + 1) & (i < nfull + KC + 1))
        def _():
            g_copy(i - KC - 1).start()

        @pl.when(i == nfull + KC)
        def _():
            for r in range(NTAIL):
                t_copy(r).start()

        @pl.when(i == 1)
        def _():
            d_g.wait_recv()
            sx[0, 2] = sum_away(0, 2)
            _remote(sx.at[0, 2:3], rx.at[0, 2:3], xs.at[0], xr.at[0], xpeer).start()

        @pl.when((i >= 2) & (i < nfull + 1))
        def _():
            j = i - 1
            d_copy(j).wait_recv()
            for k in range(3):
                sx[j, k] = sum_away(j, k)

        @pl.when(i < nfull)
        def _():
            d_copy(i).start()

        @pl.when((i >= KE) & (i < nfull + KE))
        def _():
            j = i - KE
            s = j % SLOTS
            f_copy(j).wait_recv()
            o_copy(j).start()
            acc[0] += _dot(hdd[j, 0], wdb[s], 1, 0)
            acc[1] += _dot(hdd[j, 1], wgb[s], 1, 1) + _dot(hdd[j, 2], wub[s], 1, 1)

        @pl.when((i >= 2) & (i < nfull + 1))
        def _():
            x_copy(i - 1).start()

        @pl.when((rest >= 0) & (rest < nrest))
        def _():
            for c in rest_w(rest):
                c.wait()
            s = rest % SLOTS2
            j = nfull + rest
            part[j, 0] = _dot(xc[0], wgb2[s], 1, 0)
            part[j, 1] = _dot(xc[0], wub2[s], 1, 0)
            part[j, 2] = _dot(xc[1], wdb2[s], 1, 1)

        @pl.when((rest >= 2) & (rest < nrest + 2))
        def _():
            keep_copy(rest - 2).start()

        @pl.when((rest >= 2 + NTAIL) & (rest < nrest + 2))
        def _():
            give_copy(rest - 2).start()

        @pl.when((rest >= 1) & (rest < nrest + 1))
        def _():
            r = rest - 1
            j = nfull + r
            d_copy(j).wait_recv()
            for k in range(3):
                give[r, k] = sum_away(j, k)
                keep[r, k] = part[j, k, pl.ds(own_abs, 32), :] + rdat[j, k, pl.ds(own, 32), :]

        @pl.when((rest >= 0) & (rest < nrest))
        def _():
            d_copy(nfull + rest).start()

        @pl.when((i >= KD) & (i < nfull + KD))
        def _():
            g_copy(i - KD).wait_recv()
            f_copy(i - KD).start()

        @pl.when((i >= KC) & (i < nfull + KC))
        def _():
            j = i - KC
            x_copy(j).wait_recv()
            vals = [part[j, k, pl.ds(own_abs, 32), :] + rdat[j, k, pl.ds(own, 32), :] + rx[j, k]
                    for k in range(3)]
            for k, v in enumerate(_sigmoid_parts(*vals)):
                hdd[j, k, pl.ds(own_abs, 32), :] = v

        return carry

    lax.fori_loop(1, nfull + KE, step, 0)

    cc = pltpu.make_async_copy(xc, xc_out, csem)
    cc.start()
    ac = pltpu.make_async_copy(acc, acc_out, asem)
    ac.start()

    def finish_full(j, carry):
        x_copy(j).wait_send()
        g_copy(j).wait_send()
        f_copy(j).wait_send()
        o_copy(j).wait()
        return carry

    def finish_all(j, carry):
        d_copy(j).wait_send()
        return carry

    def finish_keep(r, carry):
        keep_copy(r).wait()
        return carry

    def finish_give(r, carry):
        give_copy(r).wait()
        return carry

    lax.fori_loop(0, nfull, finish_full, 0)
    lax.fori_loop(0, nch, finish_all, 0)
    lax.fori_loop(0, nrest, finish_keep, 0)
    lax.fori_loop(NTAIL, nrest, finish_give, 0)
    for r in range(NTAIL):
        t_copy(r).wait()
    cc.wait()
    ac.wait()


def _exchange(x_loc, gy_loc, wg, wu, wd, nfull):
    dd, ff = wg.shape
    nch = ff // CW
    nrest = nch - nfull
    tok = 128
    hbm = pl.BlockSpec(memory_space=pl.ANY)
    dma = pltpu.SemaphoreType.DMA
    return pl.pallas_call(
        functools.partial(_exchange_kernel, nch, nfull),
        out_shape=(jax.ShapeDtypeStruct((2, tok, dd), F32),
                   jax.ShapeDtypeStruct((2, tok, dd), BF16),
                   jax.ShapeDtypeStruct((nfull, 3, tok, CW), BF16),
                   jax.ShapeDtypeStruct((nrest - NTAIL, 3, 32, CW), F32),
                   jax.ShapeDtypeStruct((nrest, 3, 32, CW), F32),
                   jax.ShapeDtypeStruct((NTAIL, 3, 32, CW), F32)),
        in_specs=[hbm] * 5,
        out_specs=(hbm,) * 6,
        scratch_shapes=[
            pltpu.VMEM((2, tok, dd), F32),
            pltpu.VMEM(x_loc.shape, BF16),
            pltpu.VMEM(gy_loc.shape, BF16),
            pltpu.VMEM((2, tok, dd), BF16),
            pltpu.VMEM((SLOTS, dd, CW), BF16),
            pltpu.VMEM((SLOTS, dd, CW), BF16),
            pltpu.VMEM((SLOTS, CW, dd), BF16),
            pltpu.VMEM((SLOTS2, dd, CW), BF16),
            pltpu.VMEM((SLOTS2, dd, CW), BF16),
            pltpu.VMEM((SLOTS2, CW, dd), BF16),
            pltpu.VMEM((nch, 3, tok, CW), F32),
            pltpu.VMEM((nch, 3, 64, CW), F32),
            pltpu.VMEM((nfull, 3, 32, CW), F32),
            pltpu.VMEM((nfull, 3, 32, CW), F32),
            pltpu.VMEM((nfull, 3, tok, CW), BF16),
            pltpu.VMEM((nrest, 3, 32, CW), F32),
            pltpu.VMEM((nrest, 3, 32, CW), F32),
            dma((3, SLOTS)), dma((3, SLOTS2)), dma((2, 7)), dma((2, 7)),
            dma((nch,)), dma((nch,)), dma((nfull,)), dma((nfull,)),
            dma((nfull,)), dma((nfull,)), dma((nfull,)), dma((nfull,)),
            dma((nfull,)), dma(()), dma((2, nrest)), dma(()), dma((NTAIL,)), dma((NTAIL,)),
            dma((2,)), dma(()),
        ],
        compiler_params=pltpu.CompilerParams(
            collective_id=0, has_side_effects=True, vmem_limit_bytes=67_043_328),
        cost_estimate=pl.CostEstimate(flops=12 * tok * dd * ff, bytes_accessed=6 * dd * ff,
                                      transcendentals=0),
        name="exchange",
    )(x_loc, gy_loc, wg, wu, wd)


def _finish_kernel(nfull, nrest, acc_in, keep_ref, tail_ref, got_ref, wg_ref, wu_ref, wd_ref,
                   give_out, hdd_out, give, acc, keep, got, wgb, wub, wdb, hdd,
                   wsem, isem, asem, vsem, gs, gr, fs, fr, osem):
    dp = lax.axis_index("dp")
    xi = dp // 2
    co = dp % 2
    mine = pl.multiple_of(co * 64, 64)
    own_abs = pl.multiple_of(co * 64 + xi * 32, 32)
    partner = {"dp": xi * 2 + (1 - co)}
    xpeer = {"dp": (1 - xi) * 2 + co}

    def wcopies(r):
        cols = pl.ds(pl.multiple_of((nfull + r) * CW, CW), CW)
        return (pltpu.make_async_copy(wg_ref.at[:, cols], wgb.at[r], wsem.at[0, r]),
                pltpu.make_async_copy(wu_ref.at[:, cols], wub.at[r], wsem.at[1, r]),
                pltpu.make_async_copy(wd_ref.at[cols, :], wdb.at[r], wsem.at[2, r]))

    def g_copy(r):
        blk = hdd.at[r, :, pl.ds(own_abs, 32), :]
        return _remote(blk, blk, gs.at[r], gr.at[r], xpeer)

    def f_copy(r):
        blk = hdd.at[r, :, pl.ds(mine, 64), :]
        return _remote(blk, blk, fs.at[r], fr.at[r], partner)

    def o_copy(r):
        return pltpu.make_async_copy(hdd.at[r], hdd_out.at[r], osem.at[r])

    barrier = pltpu.get_barrier_semaphore()
    for dev in (partner, xpeer):
        pl.semaphore_signal(barrier, inc=1, device_id=dev, device_id_type=pl.DeviceIdType.MESH)

    def fetch(r, carry):
        for c in wcopies(r):
            c.start()
        return carry

    def keep_in(r):
        return pltpu.make_async_copy(keep_ref.at[r], keep.at[r], isem.at[0, r])

    def got_in(r, src, at):
        return pltpu.make_async_copy(src.at[at], got.at[r], isem.at[1, r])

    for r in range(NTAIL):
        keep_in(r).start()
        got_in(r, tail_ref, r).start()

    def fetch_sums(r, carry):
        keep_in(r).start()
        got_in(r, got_ref, r - NTAIL).start()
        return carry

    lax.fori_loop(NTAIL, nrest, fetch_sums, 0)
    acopy = pltpu.make_async_copy(acc_in, acc, asem)
    acopy.start()
    lax.fori_loop(0, nrest, fetch, 0)
    pl.semaphore_wait(barrier, 2)

    def point(r, carry):
        @pl.when(r < nrest)
        def _():
            keep_in(r).wait()
            got_in(r, got_ref, 0).wait()
            vals = [keep[r, k] + got[r, k] for k in range(3)]
            for k, v in enumerate(_sigmoid_parts(*vals)):
                hdd[r, k, pl.ds(own_abs, 32), :] = v

        @pl.when(r >= 1)
        def _():
            g_copy(r - 1).start()

        return carry

    lax.fori_loop(0, nrest + 1, point, 0)
    acopy.wait()

    def step(i, carry):
        @pl.when(i < nrest)
        def _():
            g_copy(i).wait_recv()
            f_copy(i).start()

        @pl.when(i >= 1)
        def _():
            r = i - 1
            for c in wcopies(r):
                c.wait()
            f_copy(r).wait_recv()
            o_copy(r).start()
            acc[0] += _dot(hdd[r, 0], wdb[r], 1, 0)
            acc[1] += _dot(hdd[r, 1], wgb[r], 1, 1) + _dot(hdd[r, 2], wub[r], 1, 1)

        return carry

    lax.fori_loop(0, nrest + 1, step, 0)

    for t in range(2):
        for q in range(4):
            row = (q % 2) * 64 + (q // 2) * 32 + t * 16
            give[t * 4 + q] = acc[:, row:row + 16, :]
    vcopy = pltpu.make_async_copy(give, give_out, vsem)
    vcopy.start()

    def finish(r, carry):
        g_copy(r).wait_send()
        f_copy(r).wait_send()
        o_copy(r).wait()
        return carry

    lax.fori_loop(0, nrest, finish, 0)
    vcopy.wait()


def _finish(acc, keep, tail, got, wg, wu, wd):
    dd, ff = wg.shape
    nrest = keep.shape[0]
    nfull = ff // CW - nrest
    tok = acc.shape[1]
    hbm = pl.BlockSpec(memory_space=pl.ANY)
    dma = pltpu.SemaphoreType.DMA
    return pl.pallas_call(
        functools.partial(_finish_kernel, nfull, nrest),
        out_shape=(jax.ShapeDtypeStruct((8, 2, 16, dd), F32),
                   jax.ShapeDtypeStruct((nrest, 3, tok, CW), BF16)),
        in_specs=[hbm] * 7,
        out_specs=(hbm, hbm),
        scratch_shapes=[
            pltpu.VMEM((8, 2, 16, dd), F32),
            pltpu.VMEM((2, tok, dd), F32),
            pltpu.VMEM((nrest, 3, 32, CW), F32),
            pltpu.VMEM((nrest, 3, 32, CW), F32),
            pltpu.VMEM((nrest, dd, CW), BF16),
            pltpu.VMEM((nrest, dd, CW), BF16),
            pltpu.VMEM((nrest, CW, dd), BF16),
            pltpu.VMEM((nrest, 3, tok, CW), BF16),
            dma((3, nrest)), dma((2, nrest)), dma(()), dma(()), dma((nrest,)), dma((nrest,)), dma((nrest,)), dma((nrest,)),
            dma((nrest,)),
        ],
        compiler_params=pltpu.CompilerParams(
            collective_id=1, has_side_effects=True, vmem_limit_bytes=66 * 1000 * 1000),
        cost_estimate=pl.CostEstimate(flops=6 * tok * dd * nrest * CW, bytes_accessed=6 * dd * nrest * CW,
                                      transcendentals=0),
        name="finish",
    )(acc, keep, tail, got, wg, wu, wd)


def _grads_kernel(base, nch, xc_ref, hdd_ref, *refs):
    gwg_ref, gwu_ref, gwd_ref, hdd, xc, xt, og, ou, od, isem, osem, csem = refs[-12:]

    def fetch(j):
        return pltpu.make_async_copy(hdd_ref.at[j], hdd.at[j], isem.at[j])

    def put(j):
        s = j % RING
        cols = pl.ds(pl.multiple_of((base + j) * CW, CW), CW)
        return (pltpu.make_async_copy(og.at[s], gwg_ref.at[:, cols], osem.at[0, s]),
                pltpu.make_async_copy(ou.at[s], gwu_ref.at[:, cols], osem.at[1, s]),
                pltpu.make_async_copy(od.at[s], gwd_ref.at[cols, :], osem.at[2, s]))

    def start_fetch(j, carry):
        fetch(j).start()
        return carry

    ccopy = pltpu.make_async_copy(xc_ref, xc, csem)
    ccopy.start()
    lax.fori_loop(0, nch, start_fetch, 0)
    ccopy.wait()
    xt[...] = xc[0].T

    def step(j, carry):
        s = j % RING

        @pl.when(j >= RING)
        def _():
            for c in put(j - RING):
                c.wait()

        fetch(j).wait()
        og[s] = _dot(xt[...], hdd[j, 1], 1, 0)
        ou[s] = _dot(xt[...], hdd[j, 2], 1, 0)
        od[s] = _dot(hdd[j, 0], xc[1], 0, 0)
        for c in put(j):
            c.start()
        return carry

    lax.fori_loop(0, nch, step, 0)

    def drain(j, carry):
        for c in put(j):
            c.wait()
        return carry

    lax.fori_loop(nch - RING, nch, drain, 0)


def _grads(xc, hdd, base, ff, out=()):
    nch = hdd.shape[0]
    _, tok, dd = xc.shape
    hbm = pl.BlockSpec(memory_space=pl.ANY)
    dma = pltpu.SemaphoreType.DMA
    return pl.pallas_call(
        functools.partial(_grads_kernel, base, nch),
        out_shape=(jax.ShapeDtypeStruct((dd, ff), F32), jax.ShapeDtypeStruct((dd, ff), F32),
                   jax.ShapeDtypeStruct((ff, dd), F32)),
        in_specs=[hbm] * (2 + len(out)),
        out_specs=(hbm, hbm, hbm),
        input_output_aliases={2 + n: n for n in range(len(out))},
        scratch_shapes=[
            pltpu.VMEM(hdd.shape, BF16), pltpu.VMEM(xc.shape, BF16), pltpu.VMEM((dd, tok), BF16),
            pltpu.VMEM((RING, dd, CW), F32), pltpu.VMEM((RING, dd, CW), F32),
            pltpu.VMEM((RING, CW, dd), F32),
            dma((nch,)), dma((3, RING)), dma(()),
        ],
        compiler_params=pltpu.CompilerParams(vmem_limit_bytes=66_000_000 if out else GRAD_VMEM),
        cost_estimate=pl.CostEstimate(flops=6 * tok * dd * nch * CW, bytes_accessed=12 * dd * nch * CW,
                                      transcendentals=0),
        name="grads",
    )(xc, hdd, *out)


def solution(mesh):
    def local_step(x_loc, wg, wu, wd, gy_loc):
        ff = wg.shape[1]
        acc, xc, hdd, give, keep, tail = _exchange(x_loc, gy_loc, wg, wu, wd, NFULL)
        got = lax.ppermute(give, "dp", [(0, 2), (1, 3), (2, 0), (3, 1)])
        grads = _grads(xc, hdd, 0, ff)
        grads, keep = lax.optimization_barrier((grads, keep))
        give, hdd = _finish(acc, keep, tail, got, wg, wu, wd)
        got = lax.all_to_all(give, ("tp", "dp"), 0, 0, tiled=True)
        gwg, gwu, gwd = _grads(xc, hdd, NFULL, ff, grads)

        def own_rows(k, resid):
            both = [got[q, k] + got[q + 4, k] for q in range(4)]
            return (jnp.concatenate(both, axis=1) + resid.astype(F32)).astype(BF16)

        return own_rows(0, x_loc), own_rows(1, gy_loc), gwg, gwu, gwd

    row_spec = P(("dp", "tp"), None)
    up_spec = P("dp", "tp")
    down_spec = P("tp", "dp")
    return jax.shard_map(local_step, mesh=mesh,
                         in_specs=(row_spec, up_spec, up_spec, down_spec, row_spec),
                         out_specs=(row_spec, row_spec, up_spec, up_spec, down_spec),
                         check_vma=False)
```
